256 devices in a mesh: sta: 16 (over z, core), cell: 16 (over x, y).
Axes of the slice: x: 4, y: 4, z: 8, core: 2. Of those that a mesh axis runs over, the one named last changes fastest.
Arguments:
- station_xyz: float32 [3, 4096], P(None, 'sta'), may hold values from 0 to 1, as said below
- cell_xyz: float32 [3, 524288], P(None, 'cell'), may hold values from -0.6 to 1, as said below
- cell_weight: float32 [524288], P('cell'), may hold values from 0.3 to 3
- data: float32 [4096], P(('sta', 'cell')), may hold values from -6 to 6
- model_start: float32 [524288], P(('cell', 'sta')), may hold values from -6 to 6
Outputs:
- model_next: float32 [524288], P(('cell', 'sta'))
- residual_next: float32 [4096], P(('sta', 'cell'))
- search_next: float32 [524288], P(('cell', 'sta'))
The draws below stay inside these ranges and needn't reach their ends.
Inputs may be any that keep to these rules, and one draw needn't show every extreme that they name: `station_xyz`: rows 0 and 1 lie in [0, 1), row 2 in [0, 0.05]. `cell_xyz`: rows 0 and 1 lie in [0, 1), row 2 in [-0.6, -0.02].
All inputs are finite; a program needn't handle non-finite values.
Results may differ from the reference program's by a relative error of at most 0.0003.
Values sent between devices are 32-bit elements; how exact they have to be, the bound alone decides.
A program may use at most 64 MiB of HBM per device.

```python
import math
import jax
import jax.numpy as jnp
from jax import lax

STATIONS = 4096
CELLS = 524288


def draw_station_xyz(key, part):
    plane = jax.random.uniform(jax.random.fold_in(key, 11), (2, STATIONS), jnp.float32, 0.0, 1.0)
    height = jax.random.uniform(jax.random.fold_in(key, 12), (1, STATIONS), jnp.float32, 0.0, 0.05)
    return jnp.concatenate([plane, height], axis=0)


def draw_cell_xyz(key, part):
    plane = jax.random.uniform(jax.random.fold_in(key, 21), (2, CELLS), jnp.float32, 0.0, 1.0)
    depth = jax.random.uniform(jax.random.fold_in(key, 22), (1, CELLS), jnp.float32, -0.6, -0.02)
    return jnp.concatenate([plane, depth], axis=0)


def steps_of(rng, dims, pieces, least, high):
    gain = 1.0
    for axis_at, parts in pieces:
        steps = jax.random.uniform(jax.random.fold_in(jax.random.fold_in(rng, 6), axis_at), (parts,), jnp.float32, least / len(pieces), high / len(pieces))
        gain = gain * jnp.repeat(jnp.exp(steps), dims[axis_at] // parts).reshape((-1,) + (1,) * (len(dims) - 1 - axis_at))
    return gain


def noise(own_key, shape, spread, most, cuts=(), kind=jnp.bfloat16):
    entries = spread * jax.random.normal(own_key, shape, jnp.float32)
    if cuts:
        entries = entries * steps_of(own_key, shape, cuts, -0.22, 0.18)
    return jnp.clip(entries, -most, most).astype(kind)


def setup_inputs(seed: int = 0) -> dict:
    arg_keys = jax.random.split(jax.random.key(seed), 6)
    return {
        "station_xyz": draw_station_xyz(jax.random.fold_in(arg_keys[5], 71), 0),
        "cell_xyz": draw_cell_xyz(jax.random.fold_in(arg_keys[5], 71), 0),
        "cell_weight": jnp.clip(jnp.exp(math.log(3.0) - 2.3025851 * jax.random.uniform(arg_keys[2], (CELLS,), jnp.float32) ** steps_of(arg_keys[2], (CELLS,), ((0, 16),), -0.2, 0.2)), 0.3, 3.0),
        "data": noise(arg_keys[3], (STATIONS,), 1.0, 6.0, ((0, 256),), jnp.float32),
        "model_start": noise(arg_keys[4], (CELLS,), 1.0, 6.0, ((0, 256),), jnp.float32),
    }


SOFT = 0.0001

def kernel(sta, cel, wgt, scale):
    dx = sta[0][:, None] - cel[0][None, :]
    dy = sta[1][:, None] - cel[1][None, :]
    dz = sta[2][:, None] - cel[2][None, :]
    inv = lax.rsqrt(dx * dx + dy * dy + dz * dz + SOFT)
    return scale * dz * inv * inv * inv * wgt[None, :]

def blocked(cel, wgt):
    width = min(8192, cel.shape[1])
    count = cel.shape[1] // width
    return (jnp.transpose(cel.reshape(3, count, width), (1, 0, 2)), wgt.reshape(count, width), count, width)

def forward(sta, cel, wgt, vec, scale):
    cel_b, wgt_b, count, width = blocked(cel, wgt)
    vec_b = vec.reshape(count, width)

    def step(total, item):
        tile = kernel(sta, item[0], item[1], scale)
        return (total + jnp.dot(tile, item[2], precision=lax.Precision.HIGHEST), None)
    total, _ = lax.scan(step, jnp.zeros((sta.shape[1],), jnp.float32), (cel_b, wgt_b, vec_b))
    return total

def backward(sta, cel, wgt, res, scale):
    cel_b, wgt_b, count, width = blocked(cel, wgt)

    def one(item):
        tile = kernel(sta, item[0], item[1], scale)
        return jnp.dot(res, tile, precision=lax.Precision.HIGHEST)
    return lax.map(one, (cel_b, wgt_b)).reshape(-1)

def reference(station_xyz, cell_xyz, cell_weight, data, model_start):
    scale = 1.0 / math.sqrt(STATIONS * CELLS)
    residual = data - forward(station_xyz, cell_xyz, cell_weight, model_start, scale)
    gradient = backward(station_xyz, cell_xyz, cell_weight, residual, scale)
    gamma = jnp.sum(gradient * gradient)
    image = forward(station_xyz, cell_xyz, cell_weight, gradient, scale)
    delta = jnp.sum(image * image)
    alpha = gamma / delta
    model_next = model_start + alpha * gradient
    residual_next = residual - alpha * image
    gradient_next = backward(station_xyz, cell_xyz, cell_weight, residual_next, scale)
    gamma_next = jnp.sum(gradient_next * gradient_next)
    search_next = gradient_next + gamma_next / gamma * gradient
    return (model_next, residual_next, search_next)
```

```python
import functools
import math

import jax
import jax.numpy as jnp
from jax import lax
from jax.experimental import pallas as pl
from jax.experimental.pallas import tpu as pltpu
from jax.sharding import Mesh
from jax.sharding import PartitionSpec as P

STA = ("sta_0", "sta_1")
CELL = ("cell_0", "cell_1")
STA_CELL = ("sta_0", "sta_1", "cell_0", "cell_1")
CELL_STA = ("cell_0", "cell_1", "sta_0", "sta_1")

SOFT = 0.0001
LANES = 128
ROWS = 16
PIECE = ROWS * LANES
LOGICAL = pl.DeviceIdType.LOGICAL


def tree_sum(parts):
    while len(parts) > 1:
        parts = [a + b for a, b in zip(parts[::2], parts[1::2])] + parts[len(parts) // 2 * 2 :]
    return parts[0]


def body(
    nz,
    npl,
    half,
    own_len,
    scale,
    sta_ref,
    cel_ref,
    wgt_ref,
    dat_ref,
    mod_ref,
    model_out,
    res_out,
    search_out,
    tile,
    cols,
    acc,
    rcol,
    other,
    w_all,
    v_all,
    m_all,
    p1,
    rs_out,
    rs1,
    g_all,
    p2,
    dl,
    rs2,
    sc1,
    sc2,
    pad,
    send,
    recv,
):
    me = lax.axis_index(STA_CELL)
    z, q = me // npl, me % npl
    core = q // (npl // 2)
    stations = 2 * half
    groups = stations // 8
    srows = stations // LANES

    def plane_peer(d):
        return z * npl + (q + d) % npl

    def z_peer(d):
        return (z + d) % nz * npl + q

    def put(src, dst, sem, peer):
        copy = pltpu.make_async_remote_copy(
            src_ref=src,
            dst_ref=dst,
            send_sem=send.at[sem],
            recv_sem=recv.at[sem],
            device_id=peer,
            device_id_type=LOGICAL,
        )
        copy.start()

    def arrived(ref, sem):
        pltpu.make_async_copy(ref, ref, recv.at[sem]).wait()

    def left(ref, sem):
        pltpu.make_async_copy(ref, ref, send.at[sem]).wait()

    def over_z(buf, sem):
        for d in sorted(range(1, nz), key=lambda d: -min(d, nz - d)):
            put(buf.at[0], buf.at[d], sem, z_peer(d))

    def over_plane(buf, sem):
        for d in range(1, npl):
            put(buf.at[0], buf.at[d], sem, plane_peer(d))

    def others(buf):
        return buf.at[pl.ds(1, buf.shape[0] - 1)]

    barrier = pltpu.get_barrier_semaphore()
    for d in range(1, npl):
        pl.semaphore_signal(barrier, inc=1, device_id=plane_peer(d), device_id_type=LOGICAL)
    for d in range(1, nz):
        pl.semaphore_signal(barrier, inc=1, device_id=z_peer(d), device_id_type=LOGICAL)

    def place(k):
        return (z + nz - k) % nz * 2 + core

    def columns(ref, base):
        for axis in range(3):
            for part in range(half // LANES):
                row = ref[axis : axis + 1, part * LANES : (part + 1) * LANES]
                at = pl.multiple_of(base + part * LANES, LANES)
                cols[axis, pl.ds(at, LANES), :] = jnp.broadcast_to(row, (LANES, LANES)).T

    def generate(base, low, high):
        def step(n, _):
            k = n // (ROWS // 2)
            t = n % (ROWS // 2) * 2
            at = pl.multiple_of(place(k) * PIECE + t * LANES, LANES)
            cell = [
                [
                    jnp.broadcast_to(
                        cel_ref[axis : axis + 1, pl.ds(at + u * LANES, LANES)], (8, LANES)
                    )
                    for axis in range(3)
                ]
                for u in range(2)
            ]

            def group(i, _):
                rows = pl.ds(pl.multiple_of(base + i * 8, 8), 8)
                sx, sy, sz = (cols[axis, rows, :] for axis in range(3))
                for u in range(2):
                    cx, cy, cz = cell[u]
                    dx, dy, dz = sx - cx, sy - cy, sz - cz
                    inv = lax.rsqrt(dx * dx + dy * dy + dz * dz + SOFT)
                    lane = pl.ds(pl.multiple_of((t + u) * LANES, LANES), LANES)
                    tile[k, rows, lane] = dz * inv * (inv * inv)
                return 0

            lax.fori_loop(0, half // 8, group, 0, unroll=4)
            return 0

        lax.fori_loop(low * (ROWS // 2), high * (ROWS // 2), step, 0)

    def weighted(ref):
        v_all[...] = w_all[...] * ref[...]

    def forward():
        acc[...] = jnp.zeros_like(acc)

        def piece(k, _):
            vec = [
                jnp.broadcast_to(v_all[k, t : t + 1, :], (8, LANES)) for t in range(ROWS)
            ]

            def group(i, _):
                rows = pl.ds(pl.multiple_of(i * 8, 8), 8)
                acc[rows, :] += tree_sum(
                    [
                        tile[k, rows, t * LANES : (t + 1) * LANES] * vec[t]
                        for t in range(ROWS)
                    ]
                )
                return 0

            lax.fori_loop(0, groups, group, 0, unroll=4)
            return 0

        lax.fori_loop(0, nz, piece, 0)
        return [
            jnp.sum(acc[s * LANES : (s + 1) * LANES, :].T, axis=0, keepdims=True)
            for s in range(srows)
        ]

    def spread(vec):
        for s in range(srows):
            rcol[s * LANES : (s + 1) * LANES, :] = jnp.broadcast_to(
                vec[s : s + 1, :], (LANES, LANES)
            ).T

    def backward(k):
        def group(i, sums):
            rows = pl.ds(pl.multiple_of(i * 8, 8), 8)
            r = rcol[rows, :]
            return tuple(
                sums[t] + tile[k, rows, t * LANES : (t + 1) * LANES] * r for t in range(ROWS)
            )

        zero = jnp.zeros((8, LANES), jnp.float32)
        sums = lax.fori_loop(0, groups, group, (zero,) * ROWS, unroll=4)
        for t in range(ROWS):
            rs_out[k, t : t + 1, :] = jnp.sum(sums[t], axis=0, keepdims=True)

    def reduce_to_owner(buf, sem):
        order = sorted(range(1, nz), key=lambda d: -min(d, nz - d))
        for k in order:
            backward(k)
            put(rs_out.at[k], buf.at[k], sem, (z + nz - k) % nz * npl + q)
        backward(0)
        arrived(others(buf), sem)
        total = rs_out[0]
        for k in range(1, nz):
            total = total + buf[k]
        left(others(rs_out), sem)
        return w_all[0] * total

    columns(sta_ref, core * half)
    generate(core * half, 0, nz // 2)
    pl.semaphore_wait(barrier, npl - 1 + nz - 1)
    put(sta_ref, other, 0, plane_peer(npl // 2))
    m_all[0] = mod_ref[...]
    for d in sorted(range(1, nz), key=lambda d: -min(d, nz - d)):
        put(mod_ref, m_all.at[d], 1, z_peer(d))
    generate(core * half, nz // 2, nz)
    arrived(other, 0)
    columns(other, (1 - core) * half)
    generate((1 - core) * half, 0, nz)
    for k in range(nz):
        w_all[k] = wgt_ref[place(k)] * scale

    arrived(others(m_all), 1)
    weighted(m_all)
    image = jnp.concatenate(forward(), axis=0)
    pad[...] = jnp.zeros_like(pad)
    pad[0:1, 0:own_len] = dat_ref[...]
    first = q * own_len
    mine = lax.broadcasted_iota(jnp.int32, (srows, LANES), 0) == first // LANES
    own = pltpu.roll(pad[...], first % LANES, 1)[0:1, :]
    p1[0] = jnp.where(mine, own, 0.0) - image
    over_plane(p1, 2)
    arrived(others(p1), 2)
    res = jnp.sum(p1[...], axis=0)

    spread(res)
    grad = reduce_to_owner(rs1, 3)
    g_all[0] = grad
    over_z(g_all, 4)
    arrived(others(g_all), 4)

    grads = g_all[...]
    v_all[...] = w_all[...] * grads
    square = grads * grads
    square = jnp.sum(jnp.sum(square, axis=0), axis=0, keepdims=True)
    rows = forward()
    p2[0] = jnp.concatenate(rows + [square], axis=0)
    over_plane(p2, 5)
    arrived(others(p2), 5)
    total = jnp.sum(p2[...], axis=0)
    image = total[0:srows]
    gamma = jnp.sum(total[srows : srows + 1], axis=1, keepdims=True)
    dl[0] = jnp.sum(image * image, axis=0, keepdims=True)
    over_z(dl, 6)

    spread(image)
    turn = reduce_to_owner(rs2, 7)
    arrived(others(dl), 6)
    delta = jnp.sum(jnp.sum(dl[...], axis=0), axis=1, keepdims=True)
    alpha = gamma / delta
    grad_next = grad - alpha * turn
    sc1[0] = jnp.sum(grad_next * grad_next, axis=0, keepdims=True)
    over_z(sc1, 8)
    model_out[...] = mod_ref[...] + alpha * grad
    res_next = jnp.where(mine, res - alpha * image, 0.0)
    pad[0:1, :] = jnp.sum(res_next, axis=0, keepdims=True)
    res_out[...] = pltpu.roll(pad[...], (LANES - first % LANES) % LANES, 1)[0:1, :]
    arrived(others(sc1), 8)
    sc2[0] = jnp.sum(sc1[...], axis=0)
    over_plane(sc2, 9)
    arrived(others(sc2), 9)
    gamma_next = jnp.sum(jnp.sum(sc2[...], axis=0), axis=1, keepdims=True)
    search_out[...] = grad_next + gamma_next / gamma * grad

    left(other, 0)
    for buf, sem in ((m_all, 1), (p1, 2), (g_all, 4), (p2, 5), (dl, 6), (sc1, 8), (sc2, 9)):
        left(others(buf), sem)


def solution(mesh):
    shape = mesh.devices.shape
    nx = ny = math.isqrt(shape[1])
    nz = shape[0] // 2
    npl = 2 * shape[1]
    torus = Mesh(
        mesh.devices.reshape(nz, 2, nx, ny), ("sta_0", "sta_1", "cell_0", "cell_1")
    )

    def per_device(station_xyz, cell_xyz, cell_weight, data, model_start):
        half = station_xyz.shape[1]
        stations, srows = 2 * half, 2 * half // LANES
        own_len = data.shape[0]
        scale = 1.0 / math.sqrt(half * 2 * nz * cell_xyz.shape[1] * nx * ny)
        vmem = pl.BlockSpec(memory_space=pltpu.VMEM)
        f32 = jnp.float32
        cells = pltpu.VMEM((nz, ROWS, LANES), f32)
        model, res, search = pl.pallas_call(
            functools.partial(body, nz, npl, half, own_len, scale),
            out_shape=(
                jax.ShapeDtypeStruct((ROWS, LANES), f32),
                jax.ShapeDtypeStruct((1, LANES), f32),
                jax.ShapeDtypeStruct((ROWS, LANES), f32),
            ),
            in_specs=[vmem] * 5,
            out_specs=(vmem,) * 3,
            scratch_shapes=[
                pltpu.VMEM((nz, stations, PIECE), f32),
                pltpu.VMEM((3, stations, LANES), f32),
                pltpu.VMEM((stations, LANES), f32),
                pltpu.VMEM((stations, LANES), f32),
                pltpu.VMEM((3, half), f32),
                cells,
                cells,
                cells,
                pltpu.VMEM((npl, srows, LANES), f32),
                cells,
                cells,
                cells,
                pltpu.VMEM((npl, srows + 1, LANES), f32),
                pltpu.VMEM((nz, 1, LANES), f32),
                cells,
                pltpu.VMEM((nz, 1, LANES), f32),
                pltpu.VMEM((npl, 1, LANES), f32),
                pltpu.VMEM((8, LANES), f32),
                pltpu.SemaphoreType.DMA((10,)),
                pltpu.SemaphoreType.DMA((10,)),
            ],
            compiler_params=pltpu.CompilerParams(
                collective_id=0,
                has_side_effects=True,
                vmem_limit_bytes=48 * 1024 * 1024,
            ),
            name="cgls",
        )(
            station_xyz,
            cell_xyz,
            cell_weight.reshape(-1, ROWS, LANES),
            data.reshape(1, own_len),
            model_start.reshape(ROWS, LANES),
        )
        return model.reshape(-1), res[0, :own_len], search.reshape(-1)

    in_specs = (P(None, STA), P(None, CELL), P(CELL), P(STA_CELL), P(CELL_STA))
    out_specs = (P(CELL_STA), P(STA_CELL), P(CELL_STA))
    return jax.shard_map(
        per_device, mesh=torus, in_specs=in_specs, out_specs=out_specs, check_vma=False
    )
```

```python
import functools
import math

import jax
import jax.numpy as jnp
from jax import lax
from jax.experimental import pallas as pl
from jax.experimental.pallas import tpu as pltpu
from jax.sharding import Mesh
from jax.sharding import PartitionSpec as P

STA = ("sta_0", "sta_1")
CELL = ("cell_0", "cell_1")
STA_CELL = ("sta_0", "sta_1", "cell_0", "cell_1")
CELL_STA = ("cell_0", "cell_1", "sta_0", "sta_1")

SOFT = 0.0001
MID_XY = 0.5
MID_Z = -0.275
LANES = 128
ROWS = 16
PIECE = ROWS * LANES
LOGICAL = pl.DeviceIdType.LOGICAL


def tree_sum(parts):
    while len(parts) > 1:
        parts = [a + b for a, b in zip(parts[::2], parts[1::2])] + parts[len(parts) // 2 * 2 :]
    return parts[0]


def body(
    nz,
    npl,
    half,
    own_len,
    scale,
    sta_ref,
    cel_ref,
    wgt_ref,
    dat_ref,
    mod_ref,
    model_out,
    res_out,
    search_out,
    tile,
    lhs,
    rhs,
    near,
    far,
    x_pad,
    z_col,
    acc,
    rcol,
    sta,
    other,
    cel,
    dat,
    w_all,
    v_all,
    m_all,
    p1,
    rs_out,
    rs1,
    g_all,
    p2,
    dl,
    rs2,
    sc1,
    sc2,
    pad,
    send,
    recv,
    pieces,
    load,
):
    me = lax.axis_index(STA_CELL)
    z, q = me // npl, me % npl
    core = q // (npl // 2)
    stations = 2 * half
    groups = stations // 8
    srows = stations // LANES

    def plane_peer(d):
        return z * npl + (q + d) % npl

    def z_peer(d):
        return (z + d) % nz * npl + q

    def put(src, dst, sem, peer, landed=None):
        copy = pltpu.make_async_remote_copy(
            src_ref=src,
            dst_ref=dst,
            send_sem=send.at[sem],
            recv_sem=recv.at[sem] if landed is None else landed,
            device_id=peer,
            device_id_type=LOGICAL,
        )
        copy.start()

    def arrived(ref, sem):
        pltpu.make_async_copy(ref, ref, recv.at[sem]).wait()

    def left(ref, sem):
        pltpu.make_async_copy(ref, ref, send.at[sem]).wait()

    def over_z(buf, sem, group=None):
        for d in sorted(range(1, nz), key=lambda d: -min(d, nz - d)):
            landed = None if group is None else pieces.at[group, d]
            put(buf.at[0], buf.at[d], sem, z_peer(d), landed)

    def over_plane(buf, sem):
        for d in range(1, npl):
            put(buf.at[0], buf.at[d], sem, plane_peer(d))

    def others(buf):
        return buf.at[pl.ds(1, buf.shape[0] - 1)]

    barrier = pltpu.get_barrier_semaphore()
    for d in range(1, npl):
        pl.semaphore_signal(barrier, inc=1, device_id=plane_peer(d), device_id_type=LOGICAL)
    for d in range(1, nz):
        pl.semaphore_signal(barrier, inc=1, device_id=z_peer(d), device_id_type=LOGICAL)

    loads = [pltpu.make_async_copy(sta_ref, sta, load.at[0])]
    def place(k):
        return (z + nz - k) % nz * 2 + core

    for k in range(nz):
        at = pl.ds(pl.multiple_of(place(k) * PIECE, PIECE), PIECE)
        loads.append(pltpu.make_async_copy(cel_ref.at[:, at], cel.at[k], load.at[1 + k]))
    for k in range(nz):
        loads.append(pltpu.make_async_copy(wgt_ref.at[place(k)], w_all.at[k], load.at[1 + nz + k]))
    loads.append(pltpu.make_async_copy(mod_ref, m_all.at[0], load.at[1 + 2 * nz]))
    loads.append(pltpu.make_async_copy(dat_ref, dat, load.at[2 + 2 * nz]))

    def split(x):
        high = x.astype(jnp.bfloat16).astype(jnp.float32)
        rest = x - high
        mid = rest.astype(jnp.bfloat16).astype(jnp.float32)
        return high, mid, rest - mid

    def station_side(ref, base):
        axis = lax.broadcasted_iota(jnp.int32, (3, half), 0)
        s = ref[...] - jnp.where(axis == 2, MID_Z, MID_XY)
        high, mid, low = (-2.0 * part for part in split(s))
        length = split(jnp.sum(s * s, axis=0, keepdims=True))
        one = jnp.ones((1, half), jnp.float32)
        zero = jnp.zeros((1, half), jnp.float32)
        rows = [high, one, *length, one, high, one, mid, zero]
        rows += [mid, zero, high, zero, low, zero, mid, zero]
        lhs[pl.ds(base, half), :] = jnp.concatenate(rows, axis=0).T.astype(jnp.bfloat16)
        for part in range(half // LANES):
            row = ref[2:3, part * LANES : (part + 1) * LANES]
            at = pl.multiple_of(base + part * LANES, LANES)
            z_col[pl.ds(at, LANES), :] = jnp.broadcast_to(row, (LANES, LANES)).T

    def cell_side(k, _):
        x_pad[0:3, :] = cel[k]
        x_pad[4:7, :] = cel[k]
        row = lax.broadcasted_iota(jnp.int32, (8, PIECE), 0)
        mid_of = jnp.where(row % 4 == 2, MID_Z, jnp.where(row % 4 == 3, 0.0, MID_XY))
        x = x_pad[...] - mid_of
        square = x * x
        square = square + pltpu.roll(square, 1, 0)
        high, mid, low = split(x)
        length = split(square + pltpu.roll(square, 2, 0))
        first = row < 4
        last = row % 4 == 3
        parts = [
            jnp.where(last, jnp.where(first, length[0], length[1]), jnp.where(first, high, 1.0)),
            jnp.where(first, jnp.where(last, length[2], mid), high),
            jnp.where(first, mid, low),
            jnp.where(first, high, low),
        ]
        rhs[k] = jnp.concatenate(parts, axis=0).astype(jnp.bfloat16)
        return 0

    def distances(k, base, buf):
        buf[...] = jnp.dot(lhs[pl.ds(base, half), :], rhs[k], preferred_element_type=jnp.float32)

    def kernel_of(k, base, buf):
        for t in range(ROWS):
            lanes = slice(t * LANES, (t + 1) * LANES)
            dz = z_col[pl.ds(base, half), :] - cel[k, 2:3, lanes]
            inv = lax.rsqrt(buf[:, lanes])
            tile[k, pl.ds(base, half), lanes] = (dz * inv) * (inv * inv)

    def generate(base, low, high):
        def pair(j, _):
            distances(2 * j + 1, base, far)
            kernel_of(2 * j, base, near)
            distances((2 * j + 2) % nz, base, near)
            kernel_of(2 * j + 1, base, far)
            return 0

        lax.fori_loop(low // 2, high // 2, pair, 0)

    near_first = sorted(range(1, nz), key=lambda d: min(d, nz - d))

    def forward(vector):
        acc[...] = jnp.zeros_like(acc)
        for k in (0, *near_first):
            value = vector(k)
            v_all[...] = w_all[k] * value
            vec = [jnp.broadcast_to(v_all[t : t + 1, :], (8, LANES)) for t in range(ROWS)]

            def group(i, _, k=k, vec=vec):
                rows = pl.ds(pl.multiple_of(i * 8, 8), 8)
                acc[rows, :] += tree_sum(
                    [
                        tile[k, rows, t * LANES : (t + 1) * LANES] * vec[t]
                        for t in range(ROWS)
                    ]
                )
                return 0

            lax.fori_loop(0, groups, group, 0, unroll=16)
        return [
            jnp.sum(acc[s * LANES : (s + 1) * LANES, :].T, axis=0, keepdims=True)
            for s in range(srows)
        ]

    def taken(buf, group):
        def vector(k):
            if k:
                pltpu.make_async_copy(buf.at[k], buf.at[k], pieces.at[group, k]).wait()
            return buf[k]

        return vector

    def spread(vec):
        for s in range(srows):
            rcol[s * LANES : (s + 1) * LANES, :] = jnp.broadcast_to(
                vec[s : s + 1, :], (LANES, LANES)
            ).T

    def backward(k):
        def group(i, sums):
            rows = pl.ds(pl.multiple_of(i * 8, 8), 8)
            r = rcol[rows, :]
            return tuple(
                sums[t] + tile[k, rows, t * LANES : (t + 1) * LANES] * r for t in range(ROWS)
            )

        zero = jnp.zeros((8, LANES), jnp.float32)
        sums = lax.fori_loop(0, groups, group, (zero,) * ROWS, unroll=16)
        for t in range(ROWS):
            rs_out[k, t : t + 1, :] = jnp.sum(sums[t], axis=0, keepdims=True)

    def reduce_to_owner(buf, sem):
        order = sorted(range(1, nz), key=lambda d: -min(d, nz - d))
        for k in order:
            backward(k)
            put(rs_out.at[k], buf.at[k], sem, (z + nz - k) % nz * npl + q)
        backward(0)
        arrived(others(buf), sem)
        total = rs_out[0]
        for k in range(1, nz):
            total = total + buf[k]
        left(others(rs_out), sem)
        return w_all[0] * total

    for copy in loads:
        copy.start()
    x_pad[3:4, :] = jnp.full((1, PIECE), math.sqrt(SOFT), jnp.float32)
    x_pad[7:8, :] = jnp.full((1, PIECE), math.sqrt(SOFT), jnp.float32)
    base = pl.multiple_of(core * half, half)
    loads[0].wait()
    station_side(sta, base)
    for copy in loads[1 : 1 + nz]:
        copy.wait()
    lax.fori_loop(0, nz, cell_side, 0)
    distances(0, base, near)
    generate(base, 0, nz // 2)
    for copy in loads[1 + nz :]:
        copy.wait()
    pl.semaphore_wait(barrier, npl - 1 + nz - 1)
    put(sta, other, 0, plane_peer(npl // 2))
    over_z(m_all, 1, 0)
    generate(base, nz // 2, nz)
    arrived(other, 0)
    base = pl.multiple_of((1 - core) * half, half)
    station_side(other, base)
    distances(0, base, near)
    generate(base, 0, nz)
    w_all[...] = w_all[...] * scale

    image = jnp.concatenate(forward(taken(m_all, 0)), axis=0)
    pad[...] = jnp.zeros_like(pad)
    pad[0:1, 0:own_len] = dat[...]
    first = q * own_len
    mine = lax.broadcasted_iota(jnp.int32, (srows, LANES), 0) == first // LANES
    own = pltpu.roll(pad[...], first % LANES, 1)[0:1, :]
    p1[0] = jnp.where(mine, own, 0.0) - image
    over_plane(p1, 2)
    arrived(others(p1), 2)
    res = jnp.sum(p1[...], axis=0)

    spread(res)
    grad = reduce_to_owner(rs1, 3)
    g_all[0] = grad
    over_z(g_all, 4, 1)

    rows = forward(taken(g_all, 1))
    grads = g_all[...]
    square = jnp.sum(jnp.sum(grads * grads, axis=0), axis=0, keepdims=True)
    p2[0] = jnp.concatenate(rows + [square], axis=0)
    over_plane(p2, 5)
    arrived(others(p2), 5)
    total = jnp.sum(p2[...], axis=0)
    image = total[0:srows]
    gamma = jnp.sum(total[srows : srows + 1], axis=1, keepdims=True)
    dl[0] = jnp.sum(image * image, axis=0, keepdims=True)
    over_z(dl, 6)

    spread(image)
    turn = reduce_to_owner(rs2, 7)
    arrived(others(dl), 6)
    delta = jnp.sum(jnp.sum(dl[...], axis=0), axis=1, keepdims=True)
    alpha = gamma / delta
    grad_next = grad - alpha * turn
    sc1[0] = jnp.sum(grad_next * grad_next, axis=0, keepdims=True)
    over_z(sc1, 8)
    model_out[...] = m_all[0] + alpha * grad
    res_next = jnp.where(mine, res - alpha * image, 0.0)
    pad[0:1, :] = jnp.sum(res_next, axis=0, keepdims=True)
    res_out[...] = pltpu.roll(pad[...], (LANES - first % LANES) % LANES, 1)[0:1, :]
    arrived(others(sc1), 8)
    sc2[0] = jnp.sum(sc1[...], axis=0)
    over_plane(sc2, 9)
    arrived(others(sc2), 9)
    gamma_next = jnp.sum(jnp.sum(sc2[...], axis=0), axis=1, keepdims=True)
    search_out[...] = grad_next + gamma_next / gamma * grad

    left(other, 0)
    for buf, sem in ((m_all, 1), (p1, 2), (g_all, 4), (p2, 5), (dl, 6), (sc1, 8), (sc2, 9)):
        left(others(buf), sem)


def solution(mesh):
    shape = mesh.devices.shape
    nx = ny = math.isqrt(shape[1])
    nz = shape[0] // 2
    npl = 2 * shape[1]
    torus = Mesh(
        mesh.devices.reshape(nz, 2, nx, ny), ("sta_0", "sta_1", "cell_0", "cell_1")
    )

    def per_device(station_xyz, cell_xyz, cell_weight, data, model_start):
        half = station_xyz.shape[1]
        stations, srows = 2 * half, 2 * half // LANES
        own_len = data.shape[0]
        scale = 1.0 / math.sqrt(half * 2 * nz * cell_xyz.shape[1] * nx * ny)
        vmem = pl.BlockSpec(memory_space=pltpu.VMEM)
        f32 = jnp.float32
        cells = pltpu.VMEM((nz, ROWS, LANES), f32)
        model, res, search = pl.pallas_call(
            functools.partial(body, nz, npl, half, own_len, scale),
            out_shape=(
                jax.ShapeDtypeStruct((ROWS, LANES), f32),
                jax.ShapeDtypeStruct((1, LANES), f32),
                jax.ShapeDtypeStruct((ROWS, LANES), f32),
            ),
            in_specs=[pl.BlockSpec(memory_space=pltpu.HBM)] * 5,
            out_specs=(vmem,) * 3,
            scratch_shapes=[
                pltpu.VMEM((nz, stations, PIECE), f32),
                pltpu.VMEM((stations, 32), jnp.bfloat16),
                pltpu.VMEM((nz, 32, PIECE), jnp.bfloat16),
                pltpu.VMEM((half, PIECE), f32),
                pltpu.VMEM((half, PIECE), f32),
                pltpu.VMEM((8, PIECE), f32),
                pltpu.VMEM((stations, LANES), f32),
                pltpu.VMEM((stations, LANES), f32),
                pltpu.VMEM((stations, LANES), f32),
                pltpu.VMEM((3, half), f32),
                pltpu.VMEM((3, half), f32),
                pltpu.VMEM((nz, 3, PIECE), f32),
                pltpu.VMEM((1, own_len), f32),
                cells,
                pltpu.VMEM((ROWS, LANES), f32),
                cells,
                pltpu.VMEM((npl, srows, LANES), f32),
                cells,
                cells,
                cells,
                pltpu.VMEM((npl, srows + 1, LANES), f32),
                pltpu.VMEM((nz, 1, LANES), f32),
                cells,
                pltpu.VMEM((nz, 1, LANES), f32),
                pltpu.VMEM((npl, 1, LANES), f32),
                pltpu.VMEM((8, LANES), f32),
                pltpu.SemaphoreType.DMA((10,)),
                pltpu.SemaphoreType.DMA((10,)),
                pltpu.SemaphoreType.DMA((2, nz)),
                pltpu.SemaphoreType.DMA((2 * nz + 3,)),
            ],
            compiler_params=pltpu.CompilerParams(
                collective_id=0,
                has_side_effects=True,
                vmem_limit_bytes=56 * 1024 * 1024,
            ),
            name="cgls",
        )(
            station_xyz,
            cell_xyz,
            cell_weight.reshape(-1, ROWS, LANES),
            data.reshape(1, own_len),
            model_start.reshape(ROWS, LANES),
        )
        return model.reshape(-1), res[0, :own_len], search.reshape(-1)

    in_specs = (P(None, STA), P(None, CELL), P(CELL), P(STA_CELL), P(CELL_STA))
    out_specs = (P(CELL_STA), P(STA_CELL), P(CELL_STA))
    return jax.shard_map(
        per_device, mesh=torus, in_specs=in_specs, out_specs=out_specs, check_vma=False
    )
```

```python
import functools
import math

import jax
import jax.numpy as jnp
from jax import lax
from jax.experimental import pallas as pl
from jax.experimental.pallas import tpu as pltpu
from jax.sharding import Mesh
from jax.sharding import PartitionSpec as P

STA = ("sta_0", "sta_1")
CELL = ("cell_0", "cell_1")
STA_CELL = ("sta_0", "sta_1", "cell_0", "cell_1")
CELL_STA = ("cell_0", "cell_1", "sta_0", "sta_1")

SOFT = 0.0001
MID_XY = 0.5
MID_Z = -0.275
LANES = 128
ROWS = 16
PIECE = ROWS * LANES
LOGICAL = pl.DeviceIdType.LOGICAL


def tree_sum(parts):
    while len(parts) > 1:
        parts = [a + b for a, b in zip(parts[::2], parts[1::2])] + parts[len(parts) // 2 * 2 :]
    return parts[0]


def body(
    nz,
    nx,
    ny,
    half,
    own_len,
    scale,
    sta_ref,
    cel_ref,
    wgt_ref,
    dat_ref,
    mod_ref,
    model_out,
    res_out,
    search_out,
    tile,
    lhs,
    rhs,
    near,
    far,
    x_pad,
    z_col,
    acc,
    rcol,
    sta,
    other,
    cel,
    dat,
    w_all,
    v_all,
    m_all,
    p1,
    rs_out,
    rs1,
    g_all,
    p2,
    dl,
    rs2,
    sc1,
    sc2,
    pad,
    send,
    recv,
    pieces,
    load,
):
    npl = 2 * nx * ny
    me = lax.axis_index(STA_CELL)
    z, q = me // npl, me % npl
    core = q // (nx * ny)
    stations = 2 * half
    groups = stations // 8
    srows = stations // LANES

    def plane_peer(d):
        x, y = q // ny % nx, q % ny
        to_x, to_y = (x + d // ny % nx) % nx, (y + d % ny) % ny
        return z * npl + ((core + d // (nx * ny)) % 2 * nx + to_x) * ny + to_y

    def plane_hops(d):
        dx, dy = d // ny % nx, d % ny
        return min(dx, nx - dx) + min(dy, ny - dy), d // (nx * ny)

    far_first = sorted(range(1, npl), key=plane_hops, reverse=True)

    def z_peer(d):
        return (z + d) % nz * npl + q

    def put(src, dst, sem, peer, landed=None):
        copy = pltpu.make_async_remote_copy(
            src_ref=src,
            dst_ref=dst,
            send_sem=send.at[sem],
            recv_sem=recv.at[sem] if landed is None else landed,
            device_id=peer,
            device_id_type=LOGICAL,
        )
        copy.start()

    def arrived(ref, sem):
        pltpu.make_async_copy(ref, ref, recv.at[sem]).wait()

    def left(ref, sem):
        pltpu.make_async_copy(ref, ref, send.at[sem]).wait()

    def over_z(buf, sem, group=None):
        for d in sorted(range(1, nz), key=lambda d: -min(d, nz - d)):
            landed = None if group is None else pieces.at[group, d]
            put(buf.at[0], buf.at[d], sem, z_peer(d), landed)

    def over_plane(buf, sem):
        for d in far_first:
            put(buf.at[0], buf.at[d], sem, plane_peer(d))

    def others(buf):
        return buf.at[pl.ds(1, buf.shape[0] - 1)]

    loads = [pltpu.make_async_copy(sta_ref, sta, load.at[0])]
    def place(k):
        return (z + nz - k) % nz * 2 + core

    for k in range(nz):
        at = pl.ds(pl.multiple_of(place(k) * PIECE, PIECE), PIECE)
        loads.append(pltpu.make_async_copy(cel_ref.at[:, at], cel.at[k], load.at[1 + k]))
    for k in range(nz):
        loads.append(pltpu.make_async_copy(wgt_ref.at[place(k)], w_all.at[k], load.at[1 + nz + k]))
    loads.append(pltpu.make_async_copy(mod_ref, m_all.at[0], load.at[1 + 2 * nz]))
    loads.append(pltpu.make_async_copy(dat_ref, dat, load.at[2 + 2 * nz]))

    def split(x):
        high = x.astype(jnp.bfloat16).astype(jnp.float32)
        rest = x - high
        mid = rest.astype(jnp.bfloat16).astype(jnp.float32)
        return high, mid, rest - mid

    def station_side(ref, base):
        axis = lax.broadcasted_iota(jnp.int32, (3, half), 0)
        s = ref[...] - jnp.where(axis == 2, MID_Z, MID_XY)
        high, mid, low = (-2.0 * part for part in split(s))
        length = split(jnp.sum(s * s, axis=0, keepdims=True))
        one = jnp.ones((1, half), jnp.float32)
        zero = jnp.zeros((1, half), jnp.float32)
        rows = [high, one, *length, one, high, one, mid, zero]
        rows += [mid, zero, high, zero, low, zero, mid, zero]
        lhs[pl.ds(base, half), :] = jnp.concatenate(rows, axis=0).T.astype(jnp.bfloat16)
        for part in range(half // LANES):
            row = ref[2:3, part * LANES : (part + 1) * LANES]
            at = pl.multiple_of(base + part * LANES, LANES)
            z_col[pl.ds(at, LANES), :] = jnp.broadcast_to(row, (LANES, LANES)).T

    def cell_side(k):
        x_pad[k % 2, 0:3, :] = cel[k]
        x_pad[k % 2, 4:7, :] = cel[k]
        row = lax.broadcasted_iota(jnp.int32, (8, PIECE), 0)
        mid_of = jnp.where(row % 4 == 2, MID_Z, jnp.where(row % 4 == 3, 0.0, MID_XY))
        x = x_pad[k % 2] - mid_of
        square = x * x
        square = square + pltpu.roll(square, 1, 0)
        high, mid, low = split(x)
        length = split(square + pltpu.roll(square, 2, 0))
        first = row < 4
        last = row % 4 == 3
        parts = [
            jnp.where(last, jnp.where(first, length[0], length[1]), jnp.where(first, high, 1.0)),
            jnp.where(first, jnp.where(last, length[2], mid), high),
            jnp.where(first, mid, low),
            jnp.where(first, high, low),
        ]
        rhs[k] = jnp.concatenate(parts, axis=0).astype(jnp.bfloat16)

    def distances(k, base, buf):
        buf[...] = jnp.dot(lhs[pl.ds(base, half), :], rhs[k], preferred_element_type=jnp.float32)

    def kernel_of(k, base, buf):
        for t in range(ROWS):
            lanes = slice(t * LANES, (t + 1) * LANES)
            dz = z_col[pl.ds(base, half), :] - cel[k, 2:3, lanes]
            inv = lax.rsqrt(buf[:, lanes])
            tile[k, pl.ds(base, half), lanes] = (dz * inv) * (inv * inv)

    def generate(base, first, count, after):
        bufs = (near, far)
        for i in range(count):
            ahead = (first + i + 1, base) if i < count - 1 else after
            distances(*ahead, bufs[(i + 1) % 2])
            kernel_of(first + i, base, bufs[i % 2])

    near_first = sorted(range(1, nz), key=lambda d: min(d, nz - d))

    def forward(vector):
        acc[...] = jnp.zeros_like(acc)
        for k in (0, *near_first):
            value = vector(k)
            v_all[...] = w_all[k] * value
            vec = [jnp.broadcast_to(v_all[t : t + 1, :], (8, LANES)) for t in range(ROWS)]

            def group(i, _, k=k, vec=vec):
                rows = pl.ds(pl.multiple_of(i * 8, 8), 8)
                acc[rows, :] += tree_sum(
                    [
                        tile[k, rows, t * LANES : (t + 1) * LANES] * vec[t]
                        for t in range(ROWS)
                    ]
                )
                return 0

            lax.fori_loop(0, groups, group, 0, unroll=16)
        return [
            jnp.sum(acc[s * LANES : (s + 1) * LANES, :].T, axis=0, keepdims=True)
            for s in range(srows)
        ]

    def taken(buf, group):
        def vector(k):
            if k:
                pltpu.make_async_copy(buf.at[k], buf.at[k], pieces.at[group, k]).wait()
            return buf[k]

        return vector

    def spread(vec):
        for s in range(srows):
            rcol[s * LANES : (s + 1) * LANES, :] = jnp.broadcast_to(
                vec[s : s + 1, :], (LANES, LANES)
            ).T

    def backward(k):
        def group(i, sums):
            rows = pl.ds(pl.multiple_of(i * 8, 8), 8)
            r = rcol[rows, :]
            return tuple(
                sums[t] + tile[k, rows, t * LANES : (t + 1) * LANES] * r for t in range(ROWS)
            )

        zero = jnp.zeros((8, LANES), jnp.float32)
        sums = lax.fori_loop(0, groups, group, (zero,) * ROWS, unroll=16)
        for t in range(ROWS):
            rs_out[k, t : t + 1, :] = jnp.sum(sums[t], axis=0, keepdims=True)

    def reduce_to_owner(buf, sem):
        order = sorted(range(1, nz), key=lambda d: -min(d, nz - d))
        for k in order:
            backward(k)
            put(rs_out.at[k], buf.at[k], sem, (z + nz - k) % nz * npl + q)
        backward(0)
        arrived(others(buf), sem)
        total = rs_out[0]
        for k in range(1, nz):
            total = total + buf[k]
        left(others(rs_out), sem)
        return w_all[0] * total

    for copy in loads:
        copy.start()
    barrier = pltpu.get_barrier_semaphore()
    for d in range(1, npl):
        pl.semaphore_signal(barrier, inc=1, device_id=plane_peer(d), device_id_type=LOGICAL)
    for d in range(1, nz):
        pl.semaphore_signal(barrier, inc=1, device_id=z_peer(d), device_id_type=LOGICAL)
    for i in range(2):
        for row in (3, 7):
            x_pad[i, row : row + 1, :] = jnp.full((1, PIECE), math.sqrt(SOFT), jnp.float32)
    base = pl.multiple_of(core * half, half)
    for copy in loads[: 1 + nz]:
        copy.wait()
    station_side(sta, base)
    cell_side(0)
    distances(0, base, near)
    for k in range(1, nz):
        cell_side(k)
    generate(base, 0, nz // 2, (nz // 2, base))
    for copy in loads[1 + nz :]:
        copy.wait()
    pl.semaphore_wait(barrier, npl - 1 + nz - 1)
    put(sta, other, 0, plane_peer(nx * ny))
    over_z(m_all, 1, 0)
    base_2 = pl.multiple_of((1 - core) * half, half)
    generate(base, nz // 2, nz // 4, (nz // 2 + nz // 4, base))
    arrived(other, 0)
    station_side(other, base_2)
    generate(base, nz // 2 + nz // 4, nz // 4, (0, base_2))

    def half_of(j, _):
        generate(base_2, j * (nz // 2), nz // 2, ((j + 1) % 2 * (nz // 2), base_2))
        return 0

    lax.fori_loop(0, 2, half_of, 0)
    w_all[...] = w_all[...] * scale

    image = jnp.concatenate(forward(taken(m_all, 0)), axis=0)
    pad[...] = jnp.zeros_like(pad)
    pad[0:1, 0:own_len] = dat[...]
    first = q * own_len
    mine = lax.broadcasted_iota(jnp.int32, (srows, LANES), 0) == first // LANES
    own = pltpu.roll(pad[...], first % LANES, 1)[0:1, :]
    p1[0] = jnp.where(mine, own, 0.0) - image
    over_plane(p1, 2)
    arrived(others(p1), 2)
    res = jnp.sum(p1[...], axis=0)

    spread(res)
    grad = reduce_to_owner(rs1, 3)
    g_all[0] = grad
    over_z(g_all, 4, 1)

    rows = forward(taken(g_all, 1))
    grads = g_all[...]
    square = jnp.sum(jnp.sum(grads * grads, axis=0), axis=0, keepdims=True)
    p2[0] = jnp.concatenate(rows + [square], axis=0)
    over_plane(p2, 5)
    arrived(others(p2), 5)
    total = jnp.sum(p2[...], axis=0)
    image = total[0:srows]
    gamma = jnp.sum(total[srows : srows + 1], axis=1, keepdims=True)
    dl[0] = jnp.sum(image * image, axis=0, keepdims=True)
    over_z(dl, 6)

    spread(image)
    turn = reduce_to_owner(rs2, 7)
    arrived(others(dl), 6)
    delta = jnp.sum(jnp.sum(dl[...], axis=0), axis=1, keepdims=True)
    alpha = gamma / delta
    grad_next = grad - alpha * turn
    sc1[0] = jnp.sum(grad_next * grad_next, axis=0, keepdims=True)
    over_z(sc1, 8)
    model_out[...] = m_all[0] + alpha * grad
    res_next = jnp.where(mine, res - alpha * image, 0.0)
    pad[0:1, :] = jnp.sum(res_next, axis=0, keepdims=True)
    res_out[...] = pltpu.roll(pad[...], (LANES - first % LANES) % LANES, 1)[0:1, :own_len]
    arrived(others(sc1), 8)
    sc2[0] = jnp.sum(sc1[...], axis=0)
    over_plane(sc2, 9)
    arrived(others(sc2), 9)
    gamma_next = jnp.sum(jnp.sum(sc2[...], axis=0), axis=1, keepdims=True)
    search_out[...] = grad_next + gamma_next / gamma * grad

    left(other, 0)
    for buf, sem in ((m_all, 1), (p1, 2), (g_all, 4), (p2, 5), (dl, 6), (sc1, 8), (sc2, 9)):
        left(others(buf), sem)


def write_out(model, res, search, model_out, res_out, search_out, sem):
    pairs = ((model, model_out), (res, res_out), (search, search_out))
    copies = [pltpu.make_async_copy(a, b, sem.at[i]) for i, (a, b) in enumerate(pairs)]
    for copy in copies:
        copy.start()
    for copy in copies:
        copy.wait()


def solution(mesh):
    shape = mesh.devices.shape
    nx = ny = math.isqrt(shape[1])
    nz = shape[0] // 2
    torus = Mesh(
        mesh.devices.reshape(nz, 2, nx, ny), ("sta_0", "sta_1", "cell_0", "cell_1")
    )

    npl = 2 * shape[1]

    def per_device(station_xyz, cell_xyz, cell_weight, data, model_start):
        half = station_xyz.shape[1]
        stations, srows = 2 * half, 2 * half // LANES
        own_len = data.shape[0]
        scale = 1.0 / math.sqrt(half * 2 * nz * cell_xyz.shape[1] * nx * ny)
        vmem = pl.BlockSpec(memory_space=pltpu.VMEM)
        f32 = jnp.float32
        cells = pltpu.VMEM((nz, ROWS, LANES), f32)
        shapes = (
            jax.ShapeDtypeStruct((ROWS, LANES), f32),
            jax.ShapeDtypeStruct((1, own_len), f32),
            jax.ShapeDtypeStruct((ROWS, LANES), f32),
        )
        results = pl.pallas_call(
            functools.partial(body, nz, nx, ny, half, own_len, scale),
            out_shape=tuple(pltpu.VMEM(x.shape, x.dtype) for x in shapes),
            in_specs=[pl.BlockSpec(memory_space=pltpu.HBM)] * 5,
            out_specs=(vmem,) * 3,
            scratch_shapes=[
                pltpu.VMEM((nz, stations, PIECE), f32),
                pltpu.VMEM((stations, 32), jnp.bfloat16),
                pltpu.VMEM((nz, 32, PIECE), jnp.bfloat16),
                pltpu.VMEM((half, PIECE), f32),
                pltpu.VMEM((half, PIECE), f32),
                pltpu.VMEM((2, 8, PIECE), f32),
                pltpu.VMEM((stations, LANES), f32),
                pltpu.VMEM((stations, LANES), f32),
                pltpu.VMEM((stations, LANES), f32),
                pltpu.VMEM((3, half), f32),
                pltpu.VMEM((3, half), f32),
                pltpu.VMEM((nz, 3, PIECE), f32),
                pltpu.VMEM((1, own_len), f32),
                cells,
                pltpu.VMEM((ROWS, LANES), f32),
                cells,
                pltpu.VMEM((npl, srows, LANES), f32),
                cells,
                cells,
                cells,
                pltpu.VMEM((npl, srows + 1, LANES), f32),
                pltpu.VMEM((nz, 1, LANES), f32),
                cells,
                pltpu.VMEM((nz, 1, LANES), f32),
                pltpu.VMEM((npl, 1, LANES), f32),
                pltpu.VMEM((8, LANES), f32),
                pltpu.SemaphoreType.DMA((10,)),
                pltpu.SemaphoreType.DMA((10,)),
                pltpu.SemaphoreType.DMA((2, nz)),
                pltpu.SemaphoreType.DMA((2 * nz + 3,)),
            ],
            compiler_params=pltpu.CompilerParams(
                collective_id=0,
                has_side_effects=True,
                vmem_limit_bytes=56 * 1024 * 1024,
            ),
            name="cgls",
        )(
            station_xyz,
            cell_xyz,
            cell_weight.reshape(-1, ROWS, LANES),
            data.reshape(1, own_len),
            model_start.reshape(ROWS, LANES),
        )
        model, res, search = pl.pallas_call(
            write_out,
            out_shape=shapes,
            in_specs=[vmem] * 3,
            out_specs=(pl.BlockSpec(memory_space=pltpu.HBM),) * 3,
            scratch_shapes=[pltpu.SemaphoreType.DMA((3,))],
            name="write_out",
        )(*(pltpu.with_memory_space_constraint(x, pltpu.VMEM) for x in results))
        return model.reshape(-1), res.reshape(-1), search.reshape(-1)

    in_specs = (P(None, STA), P(None, CELL), P(CELL), P(STA_CELL), P(CELL_STA))
    out_specs = (P(CELL_STA), P(STA_CELL), P(CELL_STA))
    return jax.shard_map(
        per_device, mesh=torus, in_specs=in_specs, out_specs=out_specs, check_vma=False
    )
```

```python
import functools
import math

import jax
import jax.numpy as jnp
from jax import lax
from jax.experimental import pallas as pl
from jax.experimental.pallas import tpu as pltpu
from jax.sharding import Mesh
from jax.sharding import PartitionSpec as P

STA = ("sta_0", "sta_1")
CELL = ("cell_0", "cell_1")
STA_CELL = ("sta_0", "sta_1", "cell_0", "cell_1")
CELL_STA = ("cell_0", "cell_1", "sta_0", "sta_1")

SOFT = 0.0001
MID_XY = 0.5
MID_Z = -0.275
LANES = 128
ROWS = 16
PIECE = ROWS * LANES
LOGICAL = pl.DeviceIdType.LOGICAL


def tree_sum(parts):
    while len(parts) > 1:
        parts = [a + b for a, b in zip(parts[::2], parts[1::2])] + parts[len(parts) // 2 * 2 :]
    return parts[0]


def body(
    nz,
    nx,
    ny,
    half,
    own_len,
    scale,
    sta_ref,
    cel_ref,
    wgt_ref,
    dat_ref,
    mod_ref,
    model_out,
    res_out,
    search_out,
    tile,
    lhs,
    rhs,
    near,
    far,
    x_pad,
    z_col,
    acc,
    rcol,
    sta,
    other,
    cel,
    dat,
    w_all,
    v_all,
    m_all,
    p1,
    rs_out,
    rs1,
    g_all,
    p2,
    dl,
    rs2,
    sc,
    pad,
    send,
    recv,
    pieces,
    load,
):
    npl = 2 * nx * ny
    me = lax.axis_index(STA_CELL)
    z, q = me // npl, me % npl
    core = q // (nx * ny)
    stations = 2 * half
    groups = stations // 8
    srows = stations // LANES

    def plane_peer(d):
        x, y = q // ny % nx, q % ny
        to_x, to_y = (x + d // ny % nx) % nx, (y + d % ny) % ny
        return z * npl + ((core + d // (nx * ny)) % 2 * nx + to_x) * ny + to_y

    def plane_hops(d):
        dx, dy = d // ny % nx, d % ny
        return min(dx, nx - dx) + min(dy, ny - dy), d // (nx * ny)

    far_first = sorted(range(1, npl), key=plane_hops, reverse=True)

    def z_peer(d):
        return (z + d) % nz * npl + q

    def put(src, dst, sem, peer, landed=None):
        copy = pltpu.make_async_remote_copy(
            src_ref=src,
            dst_ref=dst,
            send_sem=send.at[sem],
            recv_sem=recv.at[sem] if landed is None else landed,
            device_id=peer,
            device_id_type=LOGICAL,
        )
        copy.start()

    def arrived(ref, sem):
        pltpu.make_async_copy(ref, ref, recv.at[sem]).wait()

    def left(ref, sem):
        pltpu.make_async_copy(ref, ref, send.at[sem]).wait()

    def over_z(buf, sem, group=None):
        for d in sorted(range(1, nz), key=lambda d: -min(d, nz - d)):
            landed = None if group is None else pieces.at[group, d]
            put(buf.at[0], buf.at[d], sem, z_peer(d), landed)

    def over_plane(buf, sem):
        for d in far_first:
            put(buf.at[0], buf.at[d], sem, plane_peer(d))

    def others(buf):
        return buf.at[pl.ds(1, buf.shape[0] - 1)]

    loads = [pltpu.make_async_copy(sta_ref, sta, load.at[0])]
    def place(k):
        return (z + nz - k) % nz * 2 + core

    for k in range(nz):
        at = pl.ds(pl.multiple_of(place(k) * PIECE, PIECE), PIECE)
        loads.append(pltpu.make_async_copy(cel_ref.at[:, at], cel.at[k], load.at[1 + k]))
    for k in range(nz):
        loads.append(pltpu.make_async_copy(wgt_ref.at[place(k)], w_all.at[k], load.at[1 + nz + k]))
    loads.append(pltpu.make_async_copy(mod_ref, m_all.at[0], load.at[1 + 2 * nz]))
    loads.append(pltpu.make_async_copy(dat_ref, dat, load.at[2 + 2 * nz]))

    def split(x):
        high = x.astype(jnp.bfloat16).astype(jnp.float32)
        rest = x - high
        mid = rest.astype(jnp.bfloat16).astype(jnp.float32)
        return high, mid, rest - mid

    def station_side(ref, base):
        axis = lax.broadcasted_iota(jnp.int32, (3, half), 0)
        s = ref[...] - jnp.where(axis == 2, MID_Z, MID_XY)
        high, mid, low = (-2.0 * part for part in split(s))
        length = split(jnp.sum(s * s, axis=0, keepdims=True))
        one = jnp.ones((1, half), jnp.float32)
        zero = jnp.zeros((1, half), jnp.float32)
        rows = [high, one, *length, one, high, one, mid, zero]
        rows += [mid, zero, high, zero, low, zero, mid, zero]
        lhs[pl.ds(base, half), :] = jnp.concatenate(rows, axis=0).T.astype(jnp.bfloat16)
        for part in range(half // LANES):
            row = ref[2:3, part * LANES : (part + 1) * LANES]
            at = pl.multiple_of(base + part * LANES, LANES)
            z_col[pl.ds(at, LANES), :] = jnp.broadcast_to(row, (LANES, LANES)).T

    def cell_side(k):
        x_pad[k % 2, 0:3, :] = cel[k]
        x_pad[k % 2, 4:7, :] = cel[k]
        row = lax.broadcasted_iota(jnp.int32, (8, PIECE), 0)
        mid_of = jnp.where(row % 4 == 2, MID_Z, jnp.where(row % 4 == 3, 0.0, MID_XY))
        x = x_pad[k % 2] - mid_of
        square = x * x
        square = square + pltpu.roll(square, 1, 0)
        high, mid, low = split(x)
        length = split(square + pltpu.roll(square, 2, 0))
        first = row < 4
        last = row % 4 == 3
        parts = [
            jnp.where(last, jnp.where(first, length[0], length[1]), jnp.where(first, high, 1.0)),
            jnp.where(first, jnp.where(last, length[2], mid), high),
            jnp.where(first, mid, low),
            jnp.where(first, high, low),
        ]
        rhs[k] = jnp.concatenate(parts, axis=0).astype(jnp.bfloat16)

    def distances(k, base, buf):
        buf[...] = jnp.dot(lhs[pl.ds(base, half), :], rhs[k], preferred_element_type=jnp.float32)

    def kernel_of(k, base, buf):
        for t in range(ROWS):
            lanes = slice(t * LANES, (t + 1) * LANES)
            dz = z_col[pl.ds(base, half), :] - cel[k, 2:3, lanes]
            inv = lax.rsqrt(buf[:, lanes])
            tile[k, pl.ds(base, half), lanes] = (dz * inv) * (inv * inv)

    def generate(base, first, count, after):
        bufs = (near, far)
        for i in range(count):
            ahead = (first + i + 1, base) if i < count - 1 else after
            distances(*ahead, bufs[(i + 1) % 2])
            kernel_of(first + i, base, bufs[i % 2])

    near_first = sorted(range(1, nz), key=lambda d: min(d, nz - d))

    def forward(vector):
        acc[...] = jnp.zeros_like(acc)
        for k in (0, *near_first):
            value = vector(k)
            v_all[...] = w_all[k] * value
            vec = [jnp.broadcast_to(v_all[t : t + 1, :], (8, LANES)) for t in range(ROWS)]

            def group(i, _, k=k, vec=vec):
                rows = pl.ds(pl.multiple_of(i * 8, 8), 8)
                acc[rows, :] += tree_sum(
                    [
                        tile[k, rows, t * LANES : (t + 1) * LANES] * vec[t]
                        for t in range(ROWS)
                    ]
                )
                return 0

            lax.fori_loop(0, groups, group, 0, unroll=16)
        return [
            jnp.sum(acc[s * LANES : (s + 1) * LANES, :].T, axis=0, keepdims=True)
            for s in range(srows)
        ]

    def taken(buf, group):
        def vector(k):
            if k:
                pltpu.make_async_copy(buf.at[k], buf.at[k], pieces.at[group, k]).wait()
            return buf[k]

        return vector

    def spread(vec):
        for s in range(srows):
            rcol[s * LANES : (s + 1) * LANES, :] = jnp.broadcast_to(
                vec[s : s + 1, :], (LANES, LANES)
            ).T

    def backward(k):
        def group(i, sums):
            rows = pl.ds(pl.multiple_of(i * 8, 8), 8)
            r = rcol[rows, :]
            return tuple(
                sums[t] + tile[k, rows, t * LANES : (t + 1) * LANES] * r for t in range(ROWS)
            )

        zero = jnp.zeros((8, LANES), jnp.float32)
        sums = lax.fori_loop(0, groups, group, (zero,) * ROWS, unroll=16)
        for t in range(ROWS):
            rs_out[k, t : t + 1, :] = jnp.sum(sums[t], axis=0, keepdims=True)

    def reduce_to_owner(buf, sem):
        order = sorted(range(1, nz), key=lambda d: -min(d, nz - d))
        for k in order:
            backward(k)
            put(rs_out.at[k], buf.at[k], sem, (z + nz - k) % nz * npl + q)
        backward(0)
        arrived(others(buf), sem)
        total = rs_out[0]
        for k in range(1, nz):
            total = total + buf[k]
        left(others(rs_out), sem)
        return w_all[0] * total

    for copy in loads:
        copy.start()
    barrier = pltpu.get_barrier_semaphore()
    for d in range(1, npl):
        pl.semaphore_signal(barrier, inc=1, device_id=plane_peer(d), device_id_type=LOGICAL)
    for d in range(1, nz):
        pl.semaphore_signal(barrier, inc=1, device_id=z_peer(d), device_id_type=LOGICAL)
    for i in range(2):
        for row in (3, 7):
            x_pad[i, row : row + 1, :] = jnp.full((1, PIECE), math.sqrt(SOFT), jnp.float32)
    base = pl.multiple_of(core * half, half)
    for copy in loads[: 1 + nz]:
        copy.wait()
    station_side(sta, base)
    cell_side(0)
    distances(0, base, near)
    for k in range(1, nz):
        cell_side(k)
    generate(base, 0, nz // 2, (nz // 2, base))
    for copy in loads[1 + nz :]:
        copy.wait()
    pl.semaphore_wait(barrier, npl - 1 + nz - 1)
    put(sta, other, 0, plane_peer(nx * ny))
    over_z(m_all, 1, 0)
    base_2 = pl.multiple_of((1 - core) * half, half)
    generate(base, nz // 2, nz // 4, (nz // 2 + nz // 4, base))
    arrived(other, 0)
    station_side(other, base_2)
    generate(base, nz // 2 + nz // 4, nz // 4, (0, base_2))

    def half_of(j, _):
        generate(base_2, j * (nz // 2), nz // 2, ((j + 1) % 2 * (nz // 2), base_2))
        return 0

    lax.fori_loop(0, 2, half_of, 0)
    w_all[...] = w_all[...] * scale

    image = jnp.concatenate(forward(taken(m_all, 0)), axis=0)
    pad[...] = jnp.zeros_like(pad)
    pad[0:1, 0:own_len] = dat[...]
    first = q * own_len
    mine = lax.broadcasted_iota(jnp.int32, (srows, LANES), 0) == first // LANES
    own = pltpu.roll(pad[...], first % LANES, 1)[0:1, :]
    p1[0] = jnp.where(mine, own, 0.0) - image
    over_plane(p1, 2)
    arrived(others(p1), 2)
    res = jnp.sum(p1[...], axis=0)

    spread(res)
    grad = reduce_to_owner(rs1, 3)
    g_all[0] = grad
    over_z(g_all, 4, 1)

    rows = forward(taken(g_all, 1))
    grads = g_all[...]
    square = jnp.sum(jnp.sum(grads * grads, axis=0), axis=0, keepdims=True)
    p2[0] = jnp.concatenate(rows + [square], axis=0)
    over_plane(p2, 5)
    arrived(others(p2), 5)
    total = jnp.sum(p2[...], axis=0)
    image = total[0:srows]
    gamma = jnp.sum(total[srows : srows + 1], axis=1, keepdims=True)
    dl[0] = jnp.sum(image * image, axis=0, keepdims=True)
    over_z(dl, 6)

    spread(image)
    turn = reduce_to_owner(rs2, 7)
    arrived(others(dl), 6)
    delta = jnp.sum(jnp.sum(dl[...], axis=0), axis=1, keepdims=True)
    alpha = gamma / delta
    grad_next = grad - alpha * turn
    sc[0] = jnp.sum(grad_next * grad_next, axis=0, keepdims=True)
    for dz in (*reversed(near_first), 0):
        for d in (*far_first, 0):
            if dz or d:
                peer = (z + dz) % nz * npl + plane_peer(d) - z * npl
                put(sc.at[0], sc.at[dz * npl + d], 8, peer)
    model_out[...] = m_all[0] + alpha * grad
    res_next = jnp.where(mine, res - alpha * image, 0.0)
    pad[0:1, :] = jnp.sum(res_next, axis=0, keepdims=True)
    res_out[...] = pltpu.roll(pad[...], (LANES - first % LANES) % LANES, 1)[0:1, :own_len]
    arrived(others(sc), 8)
    gamma_next = jnp.sum(jnp.sum(sc[...], axis=0), axis=1, keepdims=True)
    search_out[...] = grad_next + gamma_next / gamma * grad

    left(other, 0)
    for buf, sem in ((m_all, 1), (p1, 2), (g_all, 4), (p2, 5), (dl, 6), (sc, 8)):
        left(others(buf), sem)


def write_out(model, res, search, model_out, res_out, search_out, sem):
    pairs = ((model, model_out), (res, res_out), (search, search_out))
    copies = [pltpu.make_async_copy(a, b, sem.at[i]) for i, (a, b) in enumerate(pairs)]
    for copy in copies:
        copy.start()
    for copy in copies:
        copy.wait()


def solution(mesh):
    shape = mesh.devices.shape
    nx = ny = math.isqrt(shape[1])
    nz = shape[0] // 2
    torus = Mesh(
        mesh.devices.reshape(nz, 2, nx, ny), ("sta_0", "sta_1", "cell_0", "cell_1")
    )

    npl = 2 * shape[1]

    def per_device(station_xyz, cell_xyz, cell_weight, data, model_start):
        half = station_xyz.shape[1]
        stations, srows = 2 * half, 2 * half // LANES
        own_len = data.shape[0]
        scale = 1.0 / math.sqrt(half * 2 * nz * cell_xyz.shape[1] * nx * ny)
        vmem = pl.BlockSpec(memory_space=pltpu.VMEM)
        f32 = jnp.float32
        cells = pltpu.VMEM((nz, ROWS, LANES), f32)
        shapes = (
            jax.ShapeDtypeStruct((ROWS, LANES), f32),
            jax.ShapeDtypeStruct((1, own_len), f32),
            jax.ShapeDtypeStruct((ROWS, LANES), f32),
        )
        results = pl.pallas_call(
            functools.partial(body, nz, nx, ny, half, own_len, scale),
            out_shape=tuple(pltpu.VMEM(x.shape, x.dtype) for x in shapes),
            in_specs=[pl.BlockSpec(memory_space=pltpu.HBM)] * 5,
            out_specs=(vmem,) * 3,
            scratch_shapes=[
                pltpu.VMEM((nz, stations, PIECE), f32),
                pltpu.VMEM((stations, 32), jnp.bfloat16),
                pltpu.VMEM((nz, 32, PIECE), jnp.bfloat16),
                pltpu.VMEM((half, PIECE), f32),
                pltpu.VMEM((half, PIECE), f32),
                pltpu.VMEM((2, 8, PIECE), f32),
                pltpu.VMEM((stations, LANES), f32),
                pltpu.VMEM((stations, LANES), f32),
                pltpu.VMEM((stations, LANES), f32),
                pltpu.VMEM((3, half), f32),
                pltpu.VMEM((3, half), f32),
                pltpu.VMEM((nz, 3, PIECE), f32),
                pltpu.VMEM((1, own_len), f32),
                cells,
                pltpu.VMEM((ROWS, LANES), f32),
                cells,
                pltpu.VMEM((npl, srows, LANES), f32),
                cells,
                cells,
                cells,
                pltpu.VMEM((npl, srows + 1, LANES), f32),
                pltpu.VMEM((nz, 1, LANES), f32),
                cells,
                pltpu.VMEM((nz * npl, 1, LANES), f32),
                pltpu.VMEM((8, LANES), f32),
                pltpu.SemaphoreType.DMA((10,)),
                pltpu.SemaphoreType.DMA((10,)),
                pltpu.SemaphoreType.DMA((2, nz)),
                pltpu.SemaphoreType.DMA((2 * nz + 3,)),
            ],
            compiler_params=pltpu.CompilerParams(
                collective_id=0,
                has_side_effects=True,
                vmem_limit_bytes=56 * 1024 * 1024,
            ),
            name="cgls",
        )(
            station_xyz,
            cell_xyz,
            cell_weight.reshape(-1, ROWS, LANES),
            data.reshape(1, own_len),
            model_start.reshape(ROWS, LANES),
        )
        model, res, search = pl.pallas_call(
            write_out,
            out_shape=shapes,
            in_specs=[vmem] * 3,
            out_specs=(pl.BlockSpec(memory_space=pltpu.HBM),) * 3,
            scratch_shapes=[pltpu.SemaphoreType.DMA((3,))],
            name="write_out",
        )(*(pltpu.with_memory_space_constraint(x, pltpu.VMEM) for x in results))
        return model.reshape(-1), res.reshape(-1), search.reshape(-1)

    in_specs = (P(None, STA), P(None, CELL), P(CELL), P(STA_CELL), P(CELL_STA))
    out_specs = (P(CELL_STA), P(STA_CELL), P(CELL_STA))
    return jax.shard_map(
        per_device, mesh=torus, in_specs=in_specs, out_specs=out_specs, check_vma=False
    )
```

```python
import functools
import math

import jax
import jax.numpy as jnp
from jax import lax
from jax.experimental import pallas as pl
from jax.experimental.pallas import tpu as pltpu
from jax.sharding import Mesh
from jax.sharding import PartitionSpec as P

STA = ("sta_0", "sta_1")
CELL = ("cell_0", "cell_1")
STA_CELL = ("sta_0", "sta_1", "cell_0", "cell_1")
CELL_STA = ("cell_0", "cell_1", "sta_0", "sta_1")

SOFT = 0.0001
MID_XY = 0.5
MID_Z = -0.275
LANES = 128
ROWS = 16
PIECE = ROWS * LANES
LOGICAL = pl.DeviceIdType.LOGICAL


def tree_sum(parts):
    while len(parts) > 1:
        parts = [a + b for a, b in zip(parts[::2], parts[1::2])] + parts[len(parts) // 2 * 2 :]
    return parts[0]


def body(
    nz,
    nx,
    ny,
    half,
    own_len,
    scale,
    sta_ref,
    cel_ref,
    wgt_ref,
    dat_ref,
    mod_ref,
    model_out,
    res_out,
    search_out,
    tile,
    lhs,
    rhs,
    near,
    far,
    x_pad,
    z_col,
    acc,
    rcol,
    sta,
    other,
    cel,
    dat,
    w_all,
    v_all,
    m_all,
    p1,
    rs_out,
    rs1,
    g_all,
    p2,
    dl,
    rs2,
    sc,
    pad,
    send,
    recv,
    pieces,
    load,
):
    npl = 2 * nx * ny
    me = lax.axis_index(STA_CELL)
    z, q = me // npl, me % npl
    core = q // (nx * ny)
    stations = 2 * half
    groups = stations // 8
    srows = stations // LANES

    def plane_peer(d):
        x, y = q // ny % nx, q % ny
        to_x, to_y = (x + d // ny % nx) % nx, (y + d % ny) % ny
        return z * npl + ((core + d // (nx * ny)) % 2 * nx + to_x) * ny + to_y

    def plane_hops(d):
        dx, dy = d // ny % nx, d % ny
        return min(dx, nx - dx) + min(dy, ny - dy), d // (nx * ny)

    def far_along_z(j):
        return (nz // 2 + jnp.where(j % 2 == 1, 0 - (j + 1) // 2, j // 2)) % nz

    far_first = sorted(range(1, npl), key=plane_hops, reverse=True)

    def z_peer(d):
        return (z + d) % nz * npl + q

    def put(src, dst, sem, peer, landed=None):
        copy = pltpu.make_async_remote_copy(
            src_ref=src,
            dst_ref=dst,
            send_sem=send.at[sem],
            recv_sem=recv.at[sem] if landed is None else landed,
            device_id=peer,
            device_id_type=LOGICAL,
        )
        copy.start()

    def arrived(ref, sem):
        pltpu.make_async_copy(ref, ref, recv.at[sem]).wait()

    def left(ref, sem):
        pltpu.make_async_copy(ref, ref, send.at[sem]).wait()

    def over_z(buf, sem, group=None, near=0):
        for d in sorted(range(1, nz), key=lambda d: (min(d, nz - d) > near, -min(d, nz - d))):
            landed = None if group is None else pieces.at[group, d]
            put(buf.at[0], buf.at[d], sem, z_peer(d), landed)

    def over_plane(buf, sem):
        for d in far_first:
            put(buf.at[0], buf.at[d], sem, plane_peer(d))

    def others(buf):
        return buf.at[pl.ds(1, buf.shape[0] - 1)]

    loads = [pltpu.make_async_copy(sta_ref, sta, load.at[0])]
    def place(k):
        return (z + nz - k) % nz * 2 + core

    for k in range(nz):
        at = pl.ds(pl.multiple_of(place(k) * PIECE, PIECE), PIECE)
        loads.append(pltpu.make_async_copy(cel_ref.at[:, at], cel.at[k], load.at[1 + k]))
    for k in range(nz):
        loads.append(pltpu.make_async_copy(wgt_ref.at[place(k)], w_all.at[k], load.at[1 + nz + k]))
    loads.append(pltpu.make_async_copy(mod_ref, m_all.at[0], load.at[1 + 2 * nz]))
    loads.append(pltpu.make_async_copy(dat_ref, dat, load.at[2 + 2 * nz]))

    def split(x):
        high = x.astype(jnp.bfloat16).astype(jnp.float32)
        rest = x - high
        mid = rest.astype(jnp.bfloat16).astype(jnp.float32)
        return high, mid, rest - mid

    def station_side(ref, base):
        axis = lax.broadcasted_iota(jnp.int32, (3, half), 0)
        s = ref[...] - jnp.where(axis == 2, MID_Z, MID_XY)
        high, mid, low = (-2.0 * part for part in split(s))
        length = split(jnp.sum(s * s, axis=0, keepdims=True))
        one = jnp.ones((1, half), jnp.float32)
        zero = jnp.zeros((1, half), jnp.float32)
        rows = [high, one, *length, one, high, one, mid, zero]
        rows += [mid, zero, high, zero, low, zero, mid, zero]
        lhs[pl.ds(base, half), :] = jnp.concatenate(rows, axis=0).T.astype(jnp.bfloat16)
        for part in range(half // LANES):
            row = ref[2:3, part * LANES : (part + 1) * LANES]
            at = pl.multiple_of(base + part * LANES, LANES)
            z_col[pl.ds(at, LANES), :] = jnp.broadcast_to(row, (LANES, LANES)).T

    def cell_side(k):
        x_pad[k % 2, 0:3, :] = cel[k]
        x_pad[k % 2, 4:7, :] = cel[k]
        row = lax.broadcasted_iota(jnp.int32, (8, PIECE), 0)
        mid_of = jnp.where(row % 4 == 2, MID_Z, jnp.where(row % 4 == 3, 0.0, MID_XY))
        x = x_pad[k % 2] - mid_of
        square = x * x
        square = square + pltpu.roll(square, 1, 0)
        high, mid, low = split(x)
        length = split(square + pltpu.roll(square, 2, 0))
        first = row < 4
        last = row % 4 == 3
        parts = [
            jnp.where(last, jnp.where(first, length[0], length[1]), jnp.where(first, high, 1.0)),
            jnp.where(first, jnp.where(last, length[2], mid), high),
            jnp.where(first, mid, low),
            jnp.where(first, high, low),
        ]
        rhs[k] = jnp.concatenate(parts, axis=0).astype(jnp.bfloat16)

    def distances(k, base, buf):
        buf[...] = jnp.dot(lhs[pl.ds(base, half), :], rhs[k], preferred_element_type=jnp.float32)

    def kernel_of(k, base, buf):
        for t in range(ROWS):
            lanes = slice(t * LANES, (t + 1) * LANES)
            dz = z_col[pl.ds(base, half), :] - cel[k, 2:3, lanes]
            inv = lax.rsqrt(buf[:, lanes])
            tile[k, pl.ds(base, half), lanes] = (dz * inv) * (inv * inv)

    def generate(base, first, count, after):
        bufs = (near, far)
        for i in range(count):
            ahead = (first + i + 1, base) if i < count - 1 else after
            distances(*ahead, bufs[(i + 1) % 2])
            kernel_of(first + i, base, bufs[i % 2])

    near_first = sorted(range(1, nz), key=lambda d: min(d, nz - d))

    def forward(vector):
        acc[...] = jnp.zeros_like(acc)
        for k in (0, *near_first):
            value = vector(k)
            v_all[...] = w_all[k] * value
            vec = [jnp.broadcast_to(v_all[t : t + 1, :], (8, LANES)) for t in range(ROWS)]

            def group(i, _, k=k, vec=vec):
                rows = pl.ds(pl.multiple_of(i * 8, 8), 8)
                acc[rows, :] += tree_sum(
                    [
                        tile[k, rows, t * LANES : (t + 1) * LANES] * vec[t]
                        for t in range(ROWS)
                    ]
                )
                return 0

            lax.fori_loop(0, groups, group, 0, unroll=32)
        return [
            jnp.sum(acc[s * LANES : (s + 1) * LANES, :].T, axis=0, keepdims=True)
            for s in range(srows)
        ]

    def taken(buf, group):
        def vector(k):
            if k:
                pltpu.make_async_copy(buf.at[k], buf.at[k], pieces.at[group, k]).wait()
            return buf[k]

        return vector

    def spread(vec):
        for s in range(srows):
            rcol[s * LANES : (s + 1) * LANES, :] = jnp.broadcast_to(
                vec[s : s + 1, :], (LANES, LANES)
            ).T

    def backward(k):
        def group(i, sums):
            rows = pl.ds(pl.multiple_of(i * 8, 8), 8)
            r = rcol[rows, :]
            return tuple(
                sums[t] + tile[k, rows, t * LANES : (t + 1) * LANES] * r for t in range(ROWS)
            )

        zero = jnp.zeros((8, LANES), jnp.float32)
        sums = lax.fori_loop(0, groups, group, (zero,) * ROWS, unroll=32)
        for t in range(ROWS):
            rs_out[k, t : t + 1, :] = jnp.sum(sums[t], axis=0, keepdims=True)

    def reduce_to_owner(buf, sem):
        order = sorted(range(1, nz), key=lambda d: -min(d, nz - d))
        for k in order:
            backward(k)
            put(rs_out.at[k], buf.at[k], sem, (z + nz - k) % nz * npl + q)
        backward(0)
        arrived(others(buf), sem)
        total = rs_out[0]
        for k in range(1, nz):
            total = total + buf[k]
        left(others(rs_out), sem)
        return w_all[0] * total

    for copy in loads:
        copy.start()
    barrier = pltpu.get_barrier_semaphore()
    for d in range(1, npl):
        pl.semaphore_signal(barrier, inc=1, device_id=plane_peer(d), device_id_type=LOGICAL)
    for d in range(1, nz):
        pl.semaphore_signal(barrier, inc=1, device_id=z_peer(d), device_id_type=LOGICAL)
    for i in range(2):
        for row in (3, 7):
            x_pad[i, row : row + 1, :] = jnp.full((1, PIECE), math.sqrt(SOFT), jnp.float32)
    base = pl.multiple_of(core * half, half)
    for copy in loads[: 1 + nz]:
        copy.wait()
    station_side(sta, base)
    cell_side(0)
    distances(0, base, near)
    for k in range(1, nz):
        cell_side(k)
    generate(base, 0, nz // 2, (nz // 2, base))
    for copy in loads[1 + nz :]:
        copy.wait()
    pl.semaphore_wait(barrier, npl - 1 + nz - 1)
    put(sta, other, 0, plane_peer(nx * ny))
    over_z(m_all, 1, 0)
    base_2 = pl.multiple_of((1 - core) * half, half)
    generate(base, nz // 2, nz // 4, (nz // 2 + nz // 4, base))
    arrived(other, 0)
    station_side(other, base_2)
    generate(base, nz // 2 + nz // 4, nz // 4, (0, base_2))

    def half_of(j, _):
        generate(base_2, j * (nz // 2), nz // 2, ((j + 1) % 2 * (nz // 2), base_2))
        return 0

    lax.fori_loop(0, 2, half_of, 0)
    w_all[...] = w_all[...] * scale

    image = jnp.concatenate(forward(taken(m_all, 0)), axis=0)
    pad[...] = jnp.zeros_like(pad)
    pad[0:1, 0:own_len] = dat[...]
    first = q * own_len
    mine = lax.broadcasted_iota(jnp.int32, (srows, LANES), 0) == first // LANES
    own = pltpu.roll(pad[...], first % LANES, 1)[0:1, :]
    p1[0] = jnp.where(mine, own, 0.0) - image
    over_plane(p1, 2)
    arrived(others(p1), 2)
    res = jnp.sum(p1[...], axis=0)

    spread(res)
    grad = reduce_to_owner(rs1, 3)
    g_all[0] = grad
    over_z(g_all, 4, 1, 1)

    rows = forward(taken(g_all, 1))
    grads = g_all[...]
    square = jnp.sum(jnp.sum(grads * grads, axis=0), axis=0, keepdims=True)
    p2[0] = jnp.concatenate(rows + [square], axis=0)
    over_plane(p2, 5)
    arrived(others(p2), 5)
    total = jnp.sum(p2[...], axis=0)
    image = total[0:srows]
    gamma = jnp.sum(total[srows : srows + 1], axis=1, keepdims=True)
    dl[0] = jnp.sum(image * image, axis=0, keepdims=True)
    over_z(dl, 6)

    spread(image)
    turn = reduce_to_owner(rs2, 7)
    arrived(others(dl), 6)
    delta = jnp.sum(jnp.sum(dl[...], axis=0), axis=1, keepdims=True)
    alpha = gamma / delta
    grad_next = grad - alpha * turn
    sc[0:1, :] = jnp.sum(grad_next * grad_next, axis=0, keepdims=True)

    def scalars(j, _):
        dz = far_along_z(j)

        def to(d):
            peer = (z + dz) % nz * npl + plane_peer(d) - z * npl
            put(sc.at[pl.ds(0, 1)], sc.at[pl.ds(dz * npl + d, 1)], 8, peer)

        for d in far_first:
            to(d)
        pl.when(dz > 0)(lambda: to(0))
        return 0

    lax.fori_loop(0, nz, scalars, 0)
    model_out[...] = m_all[0] + alpha * grad
    res_next = jnp.where(mine, res - alpha * image, 0.0)
    pad[0:1, :] = jnp.sum(res_next, axis=0, keepdims=True)
    res_out[...] = pltpu.roll(pad[...], (LANES - first % LANES) % LANES, 1)[0:1, :own_len]
    arrived(others(sc), 8)
    gamma_next = jnp.sum(jnp.sum(sc[...], axis=0, keepdims=True), axis=1, keepdims=True)
    search_out[...] = grad_next + gamma_next / gamma * grad

    left(other, 0)
    for buf, sem in ((m_all, 1), (p1, 2), (g_all, 4), (p2, 5), (dl, 6), (sc, 8)):
        left(others(buf), sem)


def write_out(model, res, search, model_out, res_out, search_out, sem):
    pairs = ((model, model_out), (res, res_out), (search, search_out))
    copies = [pltpu.make_async_copy(a, b, sem.at[i]) for i, (a, b) in enumerate(pairs)]
    for copy in copies:
        copy.start()
    for copy in copies:
        copy.wait()


def solution(mesh):
    shape = mesh.devices.shape
    nx = ny = math.isqrt(shape[1])
    nz = shape[0] // 2
    torus = Mesh(
        mesh.devices.reshape(nz, 2, nx, ny), ("sta_0", "sta_1", "cell_0", "cell_1")
    )

    npl = 2 * shape[1]

    def per_device(station_xyz, cell_xyz, cell_weight, data, model_start):
        half = station_xyz.shape[1]
        stations, srows = 2 * half, 2 * half // LANES
        own_len = data.shape[0]
        scale = 1.0 / math.sqrt(half * 2 * nz * cell_xyz.shape[1] * nx * ny)
        vmem = pl.BlockSpec(memory_space=pltpu.VMEM)
        f32 = jnp.float32
        cells = pltpu.VMEM((nz, ROWS, LANES), f32)
        shapes = (
            jax.ShapeDtypeStruct((ROWS, LANES), f32),
            jax.ShapeDtypeStruct((1, own_len), f32),
            jax.ShapeDtypeStruct((ROWS, LANES), f32),
        )
        results = pl.pallas_call(
            functools.partial(body, nz, nx, ny, half, own_len, scale),
            out_shape=tuple(pltpu.VMEM(x.shape, x.dtype) for x in shapes),
            in_specs=[pl.BlockSpec(memory_space=pltpu.HBM)] * 5,
            out_specs=(vmem,) * 3,
            scratch_shapes=[
                pltpu.VMEM((nz, stations, PIECE), f32),
                pltpu.VMEM((stations, 32), jnp.bfloat16),
                pltpu.VMEM((nz, 32, PIECE), jnp.bfloat16),
                pltpu.VMEM((half, PIECE), f32),
                pltpu.VMEM((half, PIECE), f32),
                pltpu.VMEM((2, 8, PIECE), f32),
                pltpu.VMEM((stations, LANES), f32),
                pltpu.VMEM((stations, LANES), f32),
                pltpu.VMEM((stations, LANES), f32),
                pltpu.VMEM((3, half), f32),
                pltpu.VMEM((3, half), f32),
                pltpu.VMEM((nz, 3, PIECE), f32),
                pltpu.VMEM((1, own_len), f32),
                cells,
                pltpu.VMEM((ROWS, LANES), f32),
                cells,
                pltpu.VMEM((npl, srows, LANES), f32),
                cells,
                cells,
                cells,
                pltpu.VMEM((npl, srows + 1, LANES), f32),
                pltpu.VMEM((nz, 1, LANES), f32),
                cells,
                pltpu.VMEM((nz * npl, LANES), f32),
                pltpu.VMEM((8, LANES), f32),
                pltpu.SemaphoreType.DMA((10,)),
                pltpu.SemaphoreType.DMA((10,)),
                pltpu.SemaphoreType.DMA((2, nz)),
                pltpu.SemaphoreType.DMA((2 * nz + 3,)),
            ],
            compiler_params=pltpu.CompilerParams(
                collective_id=0,
                has_side_effects=True,
                vmem_limit_bytes=56 * 1024 * 1024,
            ),
            name="cgls",
        )(
            station_xyz,
            cell_xyz,
            cell_weight.reshape(-1, ROWS, LANES),
            data.reshape(1, own_len),
            model_start.reshape(ROWS, LANES),
        )
        model, res, search = pl.pallas_call(
            write_out,
            out_shape=shapes,
            in_specs=[vmem] * 3,
            out_specs=(pl.BlockSpec(memory_space=pltpu.HBM),) * 3,
            scratch_shapes=[pltpu.SemaphoreType.DMA((3,))],
            name="write_out",
        )(*(pltpu.with_memory_space_constraint(x, pltpu.VMEM) for x in results))
        return model.reshape(-1), res.reshape(-1), search.reshape(-1)

    in_specs = (P(None, STA), P(None, CELL), P(CELL), P(STA_CELL), P(CELL_STA))
    out_specs = (P(CELL_STA), P(STA_CELL), P(CELL_STA))
    return jax.shard_map(
        per_device, mesh=torus, in_specs=in_specs, out_specs=out_specs, check_vma=False
    )
```

```python
import functools
import math

import jax
import jax.numpy as jnp
from jax import lax
from jax.experimental import pallas as pl
from jax.experimental.pallas import tpu as pltpu
from jax.sharding import Mesh
from jax.sharding import PartitionSpec as P

STA = ("sta_0", "sta_1")
CELL = ("cell_0", "cell_1")
STA_CELL = ("sta_0", "sta_1", "cell_0", "cell_1")
CELL_STA = ("cell_0", "cell_1", "sta_0", "sta_1")

SOFT = 0.0001
WIDE = 512
MID_XY = 0.5
MID_Z = -0.275
LANES = 128
ROWS = 16
PIECE = ROWS * LANES
LOGICAL = pl.DeviceIdType.LOGICAL


def tree_sum(parts):
    while len(parts) > 1:
        parts = [a + b for a, b in zip(parts[::2], parts[1::2])] + parts[len(parts) // 2 * 2 :]
    return parts[0]


def body(
    nz,
    nx,
    ny,
    half,
    own_len,
    scale,
    sta_ref,
    cel_ref,
    wgt_ref,
    dat_ref,
    mod_ref,
    model_out,
    res_out,
    search_out,
    tile,
    lhs,
    rhs,
    x_pad,
    z_col,
    acc,
    rcol,
    sta,
    other,
    cel,
    dat,
    w_all,
    v_all,
    m_all,
    p1,
    rs_out,
    rs1,
    g_all,
    p2,
    dl,
    rs2,
    sc,
    pad,
    send,
    recv,
    pieces,
    load,
):
    npl = 2 * nx * ny
    me = lax.axis_index(STA_CELL)
    z, q = me // npl, me % npl
    core = q // (nx * ny)
    stations = 2 * half
    groups = stations // 8
    srows = stations // LANES

    def plane_peer(d):
        x, y = q // ny % nx, q % ny
        to_x, to_y = (x + d // ny % nx) % nx, (y + d % ny) % ny
        return z * npl + ((core + d // (nx * ny)) % 2 * nx + to_x) * ny + to_y

    def plane_hops(d):
        dx, dy = d // ny % nx, d % ny
        return min(dx, nx - dx) + min(dy, ny - dy), d // (nx * ny)

    def far_along_z(j):
        return (nz // 2 + jnp.where(j % 2 == 1, 0 - (j + 1) // 2, j // 2)) % nz

    far_first = sorted(range(1, npl), key=plane_hops, reverse=True)

    def z_peer(d):
        return (z + d) % nz * npl + q

    def put(src, dst, sem, peer, landed=None):
        copy = pltpu.make_async_remote_copy(
            src_ref=src,
            dst_ref=dst,
            send_sem=send.at[sem],
            recv_sem=recv.at[sem] if landed is None else landed,
            device_id=peer,
            device_id_type=LOGICAL,
        )
        copy.start()

    def arrived(ref, sem):
        pltpu.make_async_copy(ref, ref, recv.at[sem]).wait()

    def left(ref, sem):
        pltpu.make_async_copy(ref, ref, send.at[sem]).wait()

    def over_z(buf, sem, group=None, near=0):
        for d in sorted(range(1, nz), key=lambda d: (min(d, nz - d) > near, -min(d, nz - d))):
            landed = None if group is None else pieces.at[group, d]
            put(buf.at[0], buf.at[d], sem, z_peer(d), landed)

    def over_plane(buf, sem):
        for d in far_first:
            put(buf.at[0], buf.at[d], sem, plane_peer(d))

    def others(buf):
        return buf.at[pl.ds(1, buf.shape[0] - 1)]

    loads = [pltpu.make_async_copy(sta_ref, sta, load.at[0])]
    def place(k):
        return (z + nz - k) % nz * 2 + core

    for k in range(nz):
        at = pl.ds(pl.multiple_of(place(k) * PIECE, PIECE), PIECE)
        loads.append(pltpu.make_async_copy(cel_ref.at[:, at], cel.at[k], load.at[1 + k]))
    for k in range(nz):
        loads.append(pltpu.make_async_copy(wgt_ref.at[place(k)], w_all.at[k], load.at[1 + nz + k]))
    loads.append(pltpu.make_async_copy(mod_ref, m_all.at[0], load.at[1 + 2 * nz]))
    loads.append(pltpu.make_async_copy(dat_ref, dat, load.at[2 + 2 * nz]))

    def split(x):
        high = x.astype(jnp.bfloat16).astype(jnp.float32)
        rest = x - high
        mid = rest.astype(jnp.bfloat16).astype(jnp.float32)
        return high, mid, rest - mid

    def station_side(ref, base):
        axis = lax.broadcasted_iota(jnp.int32, (3, half), 0)
        s = ref[...] - jnp.where(axis == 2, MID_Z, MID_XY)
        high, mid, low = (-2.0 * part for part in split(s))
        length = split(jnp.sum(s * s, axis=0, keepdims=True))
        one = jnp.ones((1, half), jnp.float32)
        zero = jnp.zeros((1, half), jnp.float32)
        rows = [high, one, *length, one, high, one, mid, zero]
        rows += [mid, zero, high, zero, low, zero, mid, zero]
        lhs[pl.ds(base, half), :] = jnp.concatenate(rows, axis=0).T.astype(jnp.bfloat16)
        for part in range(half // LANES):
            row = ref[2:3, part * LANES : (part + 1) * LANES]
            at = pl.multiple_of(base + part * LANES, LANES)
            z_col[pl.ds(at, LANES), :] = jnp.broadcast_to(row, (LANES, LANES)).T

    def cell_side(k):
        x_pad[k % 2, 0:3, :] = cel[k]
        x_pad[k % 2, 4:7, :] = cel[k]
        row = lax.broadcasted_iota(jnp.int32, (8, PIECE), 0)
        mid_of = jnp.where(row % 4 == 2, MID_Z, jnp.where(row % 4 == 3, 0.0, MID_XY))
        x = x_pad[k % 2] - mid_of
        square = x * x
        square = square + pltpu.roll(square, 1, 0)
        high, mid, low = split(x)
        length = split(square + pltpu.roll(square, 2, 0))
        first = row < 4
        last = row % 4 == 3
        parts = [
            jnp.where(last, jnp.where(first, length[0], length[1]), jnp.where(first, high, 1.0)),
            jnp.where(first, jnp.where(last, length[2], mid), high),
            jnp.where(first, mid, low),
            jnp.where(first, high, low),
        ]
        rhs[k] = jnp.concatenate(parts, axis=0).astype(jnp.bfloat16)

    def kernel_of(k, base):
        for n in range(0, PIECE, WIDE):
            d2 = jnp.dot(
                lhs[pl.ds(base, half), :],
                rhs[k, :, n : n + WIDE],
                preferred_element_type=jnp.float32,
            )
            for t in range(0, WIDE, LANES):
                lanes = slice(n + t, n + t + LANES)
                dz = z_col[pl.ds(base, half), :] - cel[k, 2:3, lanes]
                inv = lax.rsqrt(d2[:, t : t + LANES])
                tile[k, pl.ds(base, half), lanes] = (dz * inv) * (inv * inv)

    def generate(base, first, count):
        for i in range(count):
            kernel_of(first + i, base)

    near_first = sorted(range(1, nz), key=lambda d: min(d, nz - d))

    def forward(vector):
        acc[...] = jnp.zeros_like(acc)
        for k in (0, *near_first):
            value = vector(k)
            v_all[...] = w_all[k] * value
            vec = [jnp.broadcast_to(v_all[t : t + 1, :], (8, LANES)) for t in range(ROWS)]

            def group(i, _, k=k, vec=vec):
                rows = pl.ds(pl.multiple_of(i * 8, 8), 8)
                acc[rows, :] += tree_sum(
                    [
                        tile[k, rows, t * LANES : (t + 1) * LANES] * vec[t]
                        for t in range(ROWS)
                    ]
                )
                return 0

            lax.fori_loop(0, groups, group, 0, unroll=32)
        return [
            jnp.sum(acc[s * LANES : (s + 1) * LANES, :].T, axis=0, keepdims=True)
            for s in range(srows)
        ]

    def taken(buf, group):
        def vector(k):
            if k:
                pltpu.make_async_copy(buf.at[k], buf.at[k], pieces.at[group, k]).wait()
            return buf[k]

        return vector

    def spread(vec):
        for s in range(srows):
            rcol[s * LANES : (s + 1) * LANES, :] = jnp.broadcast_to(
                vec[s : s + 1, :], (LANES, LANES)
            ).T

    def backward(k):
        def group(i, sums):
            rows = pl.ds(pl.multiple_of(i * 8, 8), 8)
            r = rcol[rows, :]
            return tuple(
                sums[t] + tile[k, rows, t * LANES : (t + 1) * LANES] * r for t in range(ROWS)
            )

        zero = jnp.zeros((8, LANES), jnp.float32)
        sums = lax.fori_loop(0, groups, group, (zero,) * ROWS, unroll=32)
        for t in range(ROWS):
            rs_out[k, t : t + 1, :] = jnp.sum(sums[t], axis=0, keepdims=True)

    def reduce_to_owner(buf, sem):
        order = sorted(range(1, nz), key=lambda d: -min(d, nz - d))
        for k in order:
            backward(k)
            put(rs_out.at[k], buf.at[k], sem, (z + nz - k) % nz * npl + q)
        backward(0)
        arrived(others(buf), sem)
        total = rs_out[0]
        for k in range(1, nz):
            total = total + buf[k]
        left(others(rs_out), sem)
        return w_all[0] * total

    for copy in loads:
        copy.start()
    barrier = pltpu.get_barrier_semaphore()
    for d in range(1, npl):
        pl.semaphore_signal(barrier, inc=1, device_id=plane_peer(d), device_id_type=LOGICAL)
    for d in range(1, nz):
        pl.semaphore_signal(barrier, inc=1, device_id=z_peer(d), device_id_type=LOGICAL)
    for i in range(2):
        for row in (3, 7):
            x_pad[i, row : row + 1, :] = jnp.full((1, PIECE), math.sqrt(SOFT), jnp.float32)
    base = pl.multiple_of(core * half, half)
    for copy in loads[: 1 + nz]:
        copy.wait()
    station_side(sta, base)
    for k in range(nz):
        cell_side(k)
    generate(base, 0, nz // 2)
    for copy in loads[1 + nz :]:
        copy.wait()
    pl.semaphore_wait(barrier, npl - 1 + nz - 1)
    put(sta, other, 0, plane_peer(nx * ny))
    over_z(m_all, 1, 0)
    base_2 = pl.multiple_of((1 - core) * half, half)
    generate(base, nz // 2, nz // 2)
    arrived(other, 0)
    station_side(other, base_2)

    generate(base_2, 0, nz // 2)
    pl.when(me >= 0)(lambda: generate(base_2, nz // 2, nz // 2))
    w_all[...] = w_all[...] * scale

    image = jnp.concatenate(forward(taken(m_all, 0)), axis=0)
    pad[...] = jnp.zeros_like(pad)
    pad[0:1, 0:own_len] = dat[...]
    first = q * own_len
    mine = lax.broadcasted_iota(jnp.int32, (srows, LANES), 0) == first // LANES
    own = pltpu.roll(pad[...], first % LANES, 1)[0:1, :]
    p1[0] = jnp.where(mine, own, 0.0) - image
    over_plane(p1, 2)
    arrived(others(p1), 2)
    res = jnp.sum(p1[...], axis=0)

    spread(res)
    grad = reduce_to_owner(rs1, 3)
    g_all[0] = grad
    over_z(g_all, 4, 1, 1)

    rows = forward(taken(g_all, 1))
    grads = g_all[...]
    square = jnp.sum(jnp.sum(grads * grads, axis=0), axis=0, keepdims=True)
    p2[0] = jnp.concatenate(rows + [square], axis=0)
    over_plane(p2, 5)
    arrived(others(p2), 5)
    total = jnp.sum(p2[...], axis=0)
    image = total[0:srows]
    gamma = jnp.sum(total[srows : srows + 1], axis=1, keepdims=True)
    dl[0] = jnp.sum(image * image, axis=0, keepdims=True)
    over_z(dl, 6)

    spread(image)
    turn = reduce_to_owner(rs2, 7)
    arrived(others(dl), 6)
    delta = jnp.sum(jnp.sum(dl[...], axis=0), axis=1, keepdims=True)
    alpha = gamma / delta
    grad_next = grad - alpha * turn
    sc[0:1, :] = jnp.sum(grad_next * grad_next, axis=0, keepdims=True)

    def scalars(j, _):
        dz = far_along_z(j)

        def to(d):
            peer = (z + dz) % nz * npl + plane_peer(d) - z * npl
            put(sc.at[pl.ds(0, 1)], sc.at[pl.ds(dz * npl + d, 1)], 8, peer)

        for d in far_first:
            to(d)
        pl.when(dz > 0)(lambda: to(0))
        return 0

    lax.fori_loop(0, nz, scalars, 0)
    model_out[...] = m_all[0] + alpha * grad
    res_next = jnp.where(mine, res - alpha * image, 0.0)
    pad[0:1, :] = jnp.sum(res_next, axis=0, keepdims=True)
    res_out[...] = pltpu.roll(pad[...], (LANES - first % LANES) % LANES, 1)[0:1, :own_len]
    arrived(others(sc), 8)
    gamma_next = jnp.sum(jnp.sum(sc[...], axis=0, keepdims=True), axis=1, keepdims=True)
    search_out[...] = grad_next + gamma_next / gamma * grad

    left(other, 0)
    for buf, sem in ((m_all, 1), (p1, 2), (g_all, 4), (p2, 5), (dl, 6), (sc, 8)):
        left(others(buf), sem)


def write_out(model, res, search, model_out, res_out, search_out, sem):
    pairs = ((model, model_out), (res, res_out), (search, search_out))
    copies = [pltpu.make_async_copy(a, b, sem.at[i]) for i, (a, b) in enumerate(pairs)]
    for copy in copies:
        copy.start()
    for copy in copies:
        copy.wait()


def solution(mesh):
    shape = mesh.devices.shape
    nx = ny = math.isqrt(shape[1])
    nz = shape[0] // 2
    torus = Mesh(
        mesh.devices.reshape(nz, 2, nx, ny), ("sta_0", "sta_1", "cell_0", "cell_1")
    )

    npl = 2 * shape[1]

    def per_device(station_xyz, cell_xyz, cell_weight, data, model_start):
        half = station_xyz.shape[1]
        stations, srows = 2 * half, 2 * half // LANES
        own_len = data.shape[0]
        scale = 1.0 / math.sqrt(half * 2 * nz * cell_xyz.shape[1] * nx * ny)
        vmem = pl.BlockSpec(memory_space=pltpu.VMEM)
        f32 = jnp.float32
        cells = pltpu.VMEM((nz, ROWS, LANES), f32)
        shapes = (
            jax.ShapeDtypeStruct((ROWS, LANES), f32),
            jax.ShapeDtypeStruct((1, own_len), f32),
            jax.ShapeDtypeStruct((ROWS, LANES), f32),
        )
        results = pl.pallas_call(
            functools.partial(body, nz, nx, ny, half, own_len, scale),
            out_shape=tuple(pltpu.VMEM(x.shape, x.dtype) for x in shapes),
            in_specs=[pl.BlockSpec(memory_space=pltpu.HBM)] * 5,
            out_specs=(vmem,) * 3,
            scratch_shapes=[
                pltpu.VMEM((nz, stations, PIECE), f32),
                pltpu.VMEM((stations, 32), jnp.bfloat16),
                pltpu.VMEM((nz, 32, PIECE), jnp.bfloat16),
                pltpu.VMEM((2, 8, PIECE), f32),
                pltpu.VMEM((stations, LANES), f32),
                pltpu.VMEM((stations, LANES), f32),
                pltpu.VMEM((stations, LANES), f32),
                pltpu.VMEM((3, half), f32),
                pltpu.VMEM((3, half), f32),
                pltpu.VMEM((nz, 3, PIECE), f32),
                pltpu.VMEM((1, own_len), f32),
                cells,
                pltpu.VMEM((ROWS, LANES), f32),
                cells,
                pltpu.VMEM((npl, srows, LANES), f32),
                cells,
                cells,
                cells,
                pltpu.VMEM((npl, srows + 1, LANES), f32),
                pltpu.VMEM((nz, 1, LANES), f32),
                cells,
                pltpu.VMEM((nz * npl, LANES), f32),
                pltpu.VMEM((8, LANES), f32),
                pltpu.SemaphoreType.DMA((10,)),
                pltpu.SemaphoreType.DMA((10,)),
                pltpu.SemaphoreType.DMA((2, nz)),
                pltpu.SemaphoreType.DMA((2 * nz + 3,)),
            ],
            compiler_params=pltpu.CompilerParams(
                collective_id=0,
                has_side_effects=True,
                vmem_limit_bytes=56 * 1024 * 1024,
            ),
            name="cgls",
        )(
            station_xyz,
            cell_xyz,
            cell_weight.reshape(-1, ROWS, LANES),
            data.reshape(1, own_len),
            model_start.reshape(ROWS, LANES),
        )
        model, res, search = pl.pallas_call(
            write_out,
            out_shape=shapes,
            in_specs=[vmem] * 3,
            out_specs=(pl.BlockSpec(memory_space=pltpu.HBM),) * 3,
            scratch_shapes=[pltpu.SemaphoreType.DMA((3,))],
            name="write_out",
        )(*(pltpu.with_memory_space_constraint(x, pltpu.VMEM) for x in results))
        return model.reshape(-1), res.reshape(-1), search.reshape(-1)

    in_specs = (P(None, STA), P(None, CELL), P(CELL), P(STA_CELL), P(CELL_STA))
    out_specs = (P(CELL_STA), P(STA_CELL), P(CELL_STA))
    return jax.shard_map(
        per_device, mesh=torus, in_specs=in_specs, out_specs=out_specs, check_vma=False
    )
```

```python
import functools
import math

import jax
import jax.numpy as jnp
from jax import lax
from jax.experimental import pallas as pl
from jax.experimental.pallas import tpu as pltpu
from jax.sharding import Mesh
from jax.sharding import PartitionSpec as P

STA = ("sta_0", "sta_1")
CELL = ("cell_0", "cell_1")
STA_CELL = ("sta_0", "sta_1", "cell_0", "cell_1")
CELL_STA = ("cell_0", "cell_1", "sta_0", "sta_1")

SOFT = 0.0001
MID_XY = 0.5
MID_Z = -0.275
LANES = 128
ROWS = 16
PIECE = ROWS * LANES
LOGICAL = pl.DeviceIdType.LOGICAL


def tree_sum(parts):
    while len(parts) > 1:
        parts = [a + b for a, b in zip(parts[::2], parts[1::2])] + parts[len(parts) // 2 * 2 :]
    return parts[0]


def body(
    nz,
    nx,
    ny,
    half,
    own_len,
    scale,
    sta_ref,
    cel_ref,
    wgt_ref,
    dat_ref,
    mod_ref,
    model_out,
    res_out,
    search_out,
    tile,
    lhs,
    rhs,
    near,
    far,
    x_pad,
    z_col,
    acc,
    rcol,
    sta,
    other,
    cel,
    dat,
    w_all,
    v_all,
    m_all,
    p1,
    rs_out,
    rs1,
    g_all,
    p2,
    dl,
    rs2,
    sc,
    pad,
    send,
    recv,
    pieces,
    load,
):
    npl = 2 * nx * ny
    me = lax.axis_index(STA_CELL)
    z, q = me // npl, me % npl
    core = q // (nx * ny)
    stations = 2 * half
    groups = stations // 8
    srows = stations // LANES

    def plane_peer(d):
        x, y = q // ny % nx, q % ny
        to_x, to_y = (x + d // ny % nx) % nx, (y + d % ny) % ny
        return z * npl + ((core + d // (nx * ny)) % 2 * nx + to_x) * ny + to_y

    def plane_hops(d):
        dx, dy = d // ny % nx, d % ny
        return min(dx, nx - dx) + min(dy, ny - dy), d // (nx * ny)

    def far_along_z(j):
        return (nz // 2 + jnp.where(j % 2 == 1, 0 - (j + 1) // 2, j // 2)) % nz

    far_first = sorted(range(1, npl), key=plane_hops, reverse=True)

    def z_peer(d):
        return (z + d) % nz * npl + q

    def put(src, dst, sem, peer, landed=None):
        copy = pltpu.make_async_remote_copy(
            src_ref=src,
            dst_ref=dst,
            send_sem=send.at[sem],
            recv_sem=recv.at[sem] if landed is None else landed,
            device_id=peer,
            device_id_type=LOGICAL,
        )
        copy.start()

    def arrived(ref, sem):
        pltpu.make_async_copy(ref, ref, recv.at[sem]).wait()

    def left(ref, sem):
        pltpu.make_async_copy(ref, ref, send.at[sem]).wait()

    def over_z(buf, sem, group=None, near=0):
        for d in sorted(range(1, nz), key=lambda d: (min(d, nz - d) > near, -min(d, nz - d))):
            landed = None if group is None else pieces.at[group, d]
            put(buf.at[0], buf.at[d], sem, z_peer(d), landed)

    def over_plane(buf, sem):
        for d in far_first:
            put(buf.at[0], buf.at[d], sem, plane_peer(d))

    def others(buf):
        return buf.at[pl.ds(1, buf.shape[0] - 1)]

    loads = [pltpu.make_async_copy(sta_ref, sta, load.at[0])]
    def place(k):
        return (z + nz - k) % nz * 2 + core

    for k in range(nz):
        at = pl.ds(pl.multiple_of(place(k) * PIECE, PIECE), PIECE)
        loads.append(pltpu.make_async_copy(cel_ref.at[:, at], cel.at[k], load.at[1 + k]))
    for k in range(nz):
        loads.append(pltpu.make_async_copy(wgt_ref.at[place(k)], w_all.at[k], load.at[1 + nz + k]))
    loads.append(pltpu.make_async_copy(mod_ref, m_all.at[0], load.at[1 + 2 * nz]))
    loads.append(pltpu.make_async_copy(dat_ref, dat, load.at[2 + 2 * nz]))

    def split(x):
        high = x.astype(jnp.bfloat16).astype(jnp.float32)
        rest = x - high
        mid = rest.astype(jnp.bfloat16).astype(jnp.float32)
        return high, mid, rest - mid

    def station_side(ref, base):
        axis = lax.broadcasted_iota(jnp.int32, (3, half), 0)
        s = ref[...] - jnp.where(axis == 2, MID_Z, MID_XY)
        high, mid, low = (-2.0 * part for part in split(s))
        length = split(jnp.sum(s * s, axis=0, keepdims=True))
        one = jnp.ones((1, half), jnp.float32)
        zero = jnp.zeros((1, half), jnp.float32)
        rows = [high, one, *length, one, high, one, mid, zero]
        rows += [mid, zero, high, zero, low, zero, mid, zero]
        lhs[pl.ds(base, half), :] = jnp.concatenate(rows, axis=0).T.astype(jnp.bfloat16)
        for part in range(half // LANES):
            row = ref[2:3, part * LANES : (part + 1) * LANES]
            at = pl.multiple_of(base + part * LANES, LANES)
            z_col[pl.ds(at, LANES), :] = jnp.broadcast_to(row, (LANES, LANES)).T

    def cell_side(k):
        x_pad[k % 2, 0:3, :] = cel[k]
        x_pad[k % 2, 4:7, :] = cel[k]
        row = lax.broadcasted_iota(jnp.int32, (8, PIECE), 0)
        mid_of = jnp.where(row % 4 == 2, MID_Z, jnp.where(row % 4 == 3, 0.0, MID_XY))
        x = x_pad[k % 2] - mid_of
        square = x * x
        square = square + pltpu.roll(square, 1, 0)
        high, mid, low = split(x)
        length = split(square + pltpu.roll(square, 2, 0))
        first = row < 4
        last = row % 4 == 3
        parts = [
            jnp.where(last, jnp.where(first, length[0], length[1]), jnp.where(first, high, 1.0)),
            jnp.where(first, jnp.where(last, length[2], mid), high),
            jnp.where(first, mid, low),
            jnp.where(first, high, low),
        ]
        rhs[k] = jnp.concatenate(parts, axis=0).astype(jnp.bfloat16)

    def distances(k, base, buf):
        buf[...] = jnp.dot(lhs[pl.ds(base, half), :], rhs[k], preferred_element_type=jnp.float32)

    def kernel_of(k, base, buf):
        for t in range(ROWS):
            lanes = slice(t * LANES, (t + 1) * LANES)
            dz = z_col[pl.ds(base, half), :] - cel[k, 2:3, lanes]
            inv = lax.rsqrt(buf[:, lanes])
            tile[k, pl.ds(base, half), lanes] = (dz * inv) * (inv * inv)

    def generate(base, first, count, after):
        bufs = (near, far)
        for i in range(count):
            ahead = (first + i + 1, base) if i < count - 1 else after
            distances(*ahead, bufs[(i + 1) % 2])
            kernel_of(first + i, base, bufs[i % 2])

    near_first = sorted(range(1, nz), key=lambda d: min(d, nz - d))

    def forward(vector):
        acc[...] = jnp.zeros_like(acc)
        for k in (0, *near_first):
            value = vector(k)
            v_all[...] = w_all[k] * value
            vec = [jnp.broadcast_to(v_all[t : t + 1, :], (8, LANES)) for t in range(ROWS)]

            def group(i, _, k=k, vec=vec):
                rows = pl.ds(pl.multiple_of(i * 8, 8), 8)
                acc[rows, :] += tree_sum(
                    [
                        tile[k, rows, t * LANES : (t + 1) * LANES] * vec[t]
                        for t in range(ROWS)
                    ]
                )
                return 0

            lax.fori_loop(0, groups, group, 0, unroll=32)
        return [
            jnp.sum(acc[s * LANES : (s + 1) * LANES, :].T, axis=0, keepdims=True)
            for s in range(srows)
        ]

    def taken(buf, group):
        def vector(k):
            if k:
                pltpu.make_async_copy(buf.at[k], buf.at[k], pieces.at[group, k]).wait()
            return buf[k]

        return vector

    def spread(vec):
        for s in range(srows):
            rcol[s * LANES : (s + 1) * LANES, :] = jnp.broadcast_to(
                vec[s : s + 1, :], (LANES, LANES)
            ).T

    def backward(k):
        def group(i, sums):
            rows = pl.ds(pl.multiple_of(i * 8, 8), 8)
            r = rcol[rows, :]
            return tuple(
                sums[t] + tile[k, rows, t * LANES : (t + 1) * LANES] * r for t in range(ROWS)
            )

        zero = jnp.zeros((8, LANES), jnp.float32)
        sums = lax.fori_loop(0, groups, group, (zero,) * ROWS, unroll=32)
        for t in range(ROWS):
            rs_out[k, t : t + 1, :] = jnp.sum(sums[t], axis=0, keepdims=True)

    def reduce_to_owner(buf, sem):
        order = sorted(range(1, nz), key=lambda d: -min(d, nz - d))
        for k in order:
            backward(k)
            put(rs_out.at[k], buf.at[k], sem, (z + nz - k) % nz * npl + q)
        backward(0)
        arrived(others(buf), sem)
        total = rs_out[0]
        for k in range(1, nz):
            total = total + buf[k]
        left(others(rs_out), sem)
        return w_all[0] * total

    for copy in loads:
        copy.start()
    barrier = pltpu.get_barrier_semaphore()
    for d in range(1, npl):
        pl.semaphore_signal(barrier, inc=1, device_id=plane_peer(d), device_id_type=LOGICAL)
    for d in range(1, nz):
        pl.semaphore_signal(barrier, inc=1, device_id=z_peer(d), device_id_type=LOGICAL)
    for i in range(2):
        for row in (3, 7):
            x_pad[i, row : row + 1, :] = jnp.full((1, PIECE), math.sqrt(SOFT), jnp.float32)
    base = pl.multiple_of(core * half, half)
    loads[0].wait()
    station_side(sta, base)
    for k in range(nz):
        loads[1 + k].wait()
    cell_side(0)
    distances(0, base, near)
    for k in range(1, nz):
        cell_side(k)
    generate(base, 0, nz // 2, (nz // 2, base))
    for copy in loads[1 + nz :]:
        copy.wait()
    pad[...] = jnp.zeros_like(pad)
    pad[0:1, 0:own_len] = dat[...]
    first = q * own_len
    mine = lax.broadcasted_iota(jnp.int32, (srows, LANES), 0) == first // LANES
    own = pltpu.roll(pad[...], first % LANES, 1)[0:1, :]
    p1[0] = jnp.where(mine, own, 0.0)
    w_all[...] = w_all[...] * scale
    pl.semaphore_wait(barrier, npl - 1 + nz - 1)
    put(sta, other, 0, plane_peer(nx * ny))
    over_z(m_all, 1, 0)
    base_2 = pl.multiple_of((1 - core) * half, half)
    generate(base, nz // 2, nz // 4, (nz // 2 + nz // 4, base))
    arrived(other, 0)
    station_side(other, base_2)
    generate(base, nz // 2 + nz // 4, nz // 4, (0, base_2))

    def half_of(j, _):
        generate(base_2, j * (nz // 2), nz // 2, ((j + 1) % 2 * (nz // 2), base_2))
        return 0

    lax.fori_loop(0, 2, half_of, 0)

    image = jnp.concatenate(forward(taken(m_all, 0)), axis=0)
    p1[0] = p1[0] - image
    over_plane(p1, 2)
    arrived(others(p1), 2)
    res = jnp.sum(p1[...], axis=0)

    spread(res)
    grad = reduce_to_owner(rs1, 3)
    g_all[0] = grad
    over_z(g_all, 4, 1, 1)

    rows = forward(taken(g_all, 1))
    grads = g_all[...]
    square = jnp.sum(jnp.sum(grads * grads, axis=0), axis=0, keepdims=True)
    p2[0] = jnp.concatenate(rows + [square], axis=0)
    over_plane(p2, 5)
    arrived(others(p2), 5)
    total = jnp.sum(p2[...], axis=0)
    image = total[0:srows]
    gamma = jnp.sum(total[srows : srows + 1], axis=1, keepdims=True)
    dl[0] = jnp.sum(image * image, axis=0, keepdims=True)
    over_z(dl, 6)

    spread(image)
    turn = reduce_to_owner(rs2, 7)
    arrived(others(dl), 6)
    delta = jnp.sum(jnp.sum(dl[...], axis=0), axis=1, keepdims=True)
    alpha = gamma / delta
    grad_next = grad - alpha * turn
    sc[0:1, :] = jnp.sum(grad_next * grad_next, axis=0, keepdims=True)

    def scalars(j, _):
        dz = far_along_z(j)

        def to(d):
            peer = (z + dz) % nz * npl + plane_peer(d) - z * npl
            put(sc.at[pl.ds(0, 1)], sc.at[pl.ds(dz * npl + d, 1)], 8, peer)

        for d in far_first:
            to(d)
        pl.when(dz > 0)(lambda: to(0))
        return 0

    lax.fori_loop(0, nz, scalars, 0)
    model_out[...] = m_all[0] + alpha * grad
    res_next = jnp.where(mine, res - alpha * image, 0.0)
    pad[0:1, :] = jnp.sum(res_next, axis=0, keepdims=True)
    res_out[...] = pltpu.roll(pad[...], (LANES - first % LANES) % LANES, 1)[0:1, :own_len]
    arrived(others(sc), 8)
    gamma_next = jnp.sum(jnp.sum(sc[...], axis=0, keepdims=True), axis=1, keepdims=True)
    search_out[...] = grad_next + gamma_next / gamma * grad

    left(other, 0)
    for buf, sem in ((m_all, 1), (p1, 2), (g_all, 4), (p2, 5), (dl, 6), (sc, 8)):
        left(others(buf), sem)


def write_out(model, res, search, model_out, res_out, search_out, sem):
    pairs = ((model, model_out), (res, res_out), (search, search_out))
    copies = [pltpu.make_async_copy(a, b, sem.at[i]) for i, (a, b) in enumerate(pairs)]
    for copy in copies:
        copy.start()
    for copy in copies:
        copy.wait()


def solution(mesh):
    shape = mesh.devices.shape
    nx = ny = math.isqrt(shape[1])
    nz = shape[0] // 2
    torus = Mesh(
        mesh.devices.reshape(nz, 2, nx, ny), ("sta_0", "sta_1", "cell_0", "cell_1")
    )

    npl = 2 * shape[1]

    def per_device(station_xyz, cell_xyz, cell_weight, data, model_start):
        half = station_xyz.shape[1]
        stations, srows = 2 * half, 2 * half // LANES
        own_len = data.shape[0]
        scale = 1.0 / math.sqrt(half * 2 * nz * cell_xyz.shape[1] * nx * ny)
        vmem = pl.BlockSpec(memory_space=pltpu.VMEM)
        f32 = jnp.float32
        cells = pltpu.VMEM((nz, ROWS, LANES), f32)
        shapes = (
            jax.ShapeDtypeStruct((ROWS, LANES), f32),
            jax.ShapeDtypeStruct((1, own_len), f32),
            jax.ShapeDtypeStruct((ROWS, LANES), f32),
        )
        results = pl.pallas_call(
            functools.partial(body, nz, nx, ny, half, own_len, scale),
            out_shape=tuple(pltpu.VMEM(x.shape, x.dtype) for x in shapes),
            in_specs=[pl.BlockSpec(memory_space=pltpu.HBM)] * 5,
            out_specs=(vmem,) * 3,
            scratch_shapes=[
                pltpu.VMEM((nz, stations, PIECE), f32),
                pltpu.VMEM((stations, 32), jnp.bfloat16),
                pltpu.VMEM((nz, 32, PIECE), jnp.bfloat16),
                pltpu.VMEM((half, PIECE), f32),
                pltpu.VMEM((half, PIECE), f32),
                pltpu.VMEM((2, 8, PIECE), f32),
                pltpu.VMEM((stations, LANES), f32),
                pltpu.VMEM((stations, LANES), f32),
                pltpu.VMEM((stations, LANES), f32),
                pltpu.VMEM((3, half), f32),
                pltpu.VMEM((3, half), f32),
                pltpu.VMEM((nz, 3, PIECE), f32),
                pltpu.VMEM((1, own_len), f32),
                cells,
                pltpu.VMEM((ROWS, LANES), f32),
                cells,
                pltpu.VMEM((npl, srows, LANES), f32),
                cells,
                cells,
                cells,
                pltpu.VMEM((npl, srows + 1, LANES), f32),
                pltpu.VMEM((nz, 1, LANES), f32),
                cells,
                pltpu.VMEM((nz * npl, LANES), f32),
                pltpu.VMEM((8, LANES), f32),
                pltpu.SemaphoreType.DMA((10,)),
                pltpu.SemaphoreType.DMA((10,)),
                pltpu.SemaphoreType.DMA((2, nz)),
                pltpu.SemaphoreType.DMA((2 * nz + 3,)),
            ],
            compiler_params=pltpu.CompilerParams(
                collective_id=0,
                has_side_effects=True,
                vmem_limit_bytes=56 * 1024 * 1024,
            ),
            name="cgls",
        )(
            station_xyz,
            cell_xyz,
            cell_weight.reshape(-1, ROWS, LANES),
            data.reshape(1, own_len),
            model_start.reshape(ROWS, LANES),
        )
        model, res, search = pl.pallas_call(
            write_out,
            out_shape=shapes,
            in_specs=[vmem] * 3,
            out_specs=(pl.BlockSpec(memory_space=pltpu.HBM),) * 3,
            scratch_shapes=[pltpu.SemaphoreType.DMA((3,))],
            name="write_out",
        )(*(pltpu.with_memory_space_constraint(x, pltpu.VMEM) for x in results))
        return model.reshape(-1), res.reshape(-1), search.reshape(-1)

    in_specs = (P(None, STA), P(None, CELL), P(CELL), P(STA_CELL), P(CELL_STA))
    out_specs = (P(CELL_STA), P(STA_CELL), P(CELL_STA))
    return jax.shard_map(
        per_device, mesh=torus, in_specs=in_specs, out_specs=out_specs, check_vma=False
    )
```

```python
import functools
import math

import jax
import jax.numpy as jnp
from jax import lax
from jax.experimental import pallas as pl
from jax.experimental.pallas import tpu as pltpu
from jax.sharding import Mesh
from jax.sharding import PartitionSpec as P

STA = ("sta_0", "sta_1")
CELL = ("cell_0", "cell_1")
STA_CELL = ("sta_0", "sta_1", "cell_0", "cell_1")
CELL_STA = ("cell_0", "cell_1", "sta_0", "sta_1")

SOFT = 0.0001
MID_XY = 0.5
MID_Z = -0.275
LANES = 128
ROWS = 16
PIECE = ROWS * LANES
LOGICAL = pl.DeviceIdType.LOGICAL


def tree_sum(parts):
    while len(parts) > 1:
        parts = [a + b for a, b in zip(parts[::2], parts[1::2])] + parts[len(parts) // 2 * 2 :]
    return parts[0]


def body(
    nz,
    nx,
    ny,
    half,
    own_len,
    scale,
    sta_ref,
    cel_ref,
    wgt_ref,
    dat_ref,
    mod_ref,
    model_out,
    res_out,
    search_out,
    tile,
    lhs,
    rhs,
    near,
    far,
    x_pad,
    z_col,
    acc,
    rcol,
    sta,
    other,
    cel,
    dat,
    w_all,
    v_all,
    m_all,
    p1,
    rs_out,
    rs1,
    g_all,
    p2,
    dl,
    rs2,
    sc,
    pad,
    send,
    recv,
    pieces,
    load,
):
    npl = 2 * nx * ny
    me = lax.axis_index(STA_CELL)
    z, q = me // npl, me % npl
    core = q // (nx * ny)
    stations = 2 * half
    groups = stations // 8
    srows = stations // LANES

    def plane_peer(d):
        x, y = q // ny % nx, q % ny
        to_x, to_y = (x + d // ny % nx) % nx, (y + d % ny) % ny
        return z * npl + ((core + d // (nx * ny)) % 2 * nx + to_x) * ny + to_y

    def plane_hops(d):
        dx, dy = d // ny % nx, d % ny
        return min(dx, nx - dx) + min(dy, ny - dy), d // (nx * ny)

    def far_along_z(j):
        return (nz // 2 + jnp.where(j % 2 == 1, 0 - (j + 1) // 2, j // 2)) % nz

    far_first = sorted(range(1, npl), key=plane_hops, reverse=True)

    def z_peer(d):
        return (z + d) % nz * npl + q

    def put(src, dst, sem, peer, landed=None):
        copy = pltpu.make_async_remote_copy(
            src_ref=src,
            dst_ref=dst,
            send_sem=send.at[sem],
            recv_sem=recv.at[sem] if landed is None else landed,
            device_id=peer,
            device_id_type=LOGICAL,
        )
        copy.start()

    def arrived(ref, sem):
        pltpu.make_async_copy(ref, ref, recv.at[sem]).wait()

    def left(ref, sem):
        pltpu.make_async_copy(ref, ref, send.at[sem]).wait()

    def over_z(buf, sem, group=None, near=0):
        for d in sorted(range(1, nz), key=lambda d: (min(d, nz - d) > near, -min(d, nz - d))):
            landed = None if group is None else pieces.at[group, d]
            put(buf.at[0], buf.at[d], sem, z_peer(d), landed)

    def over_plane(buf, sem):
        for d in far_first:
            put(buf.at[0], buf.at[d], sem, plane_peer(d))

    def others(buf):
        return buf.at[pl.ds(1, buf.shape[0] - 1)]

    loads = [pltpu.make_async_copy(sta_ref, sta, load.at[0])]
    def place(k):
        return (z + nz - k) % nz * 2 + core

    for k in range(nz):
        at = pl.ds(pl.multiple_of(place(k) * PIECE, PIECE), PIECE)
        loads.append(pltpu.make_async_copy(cel_ref.at[:, at], cel.at[k], load.at[1 + k]))
    for k in range(nz):
        loads.append(pltpu.make_async_copy(wgt_ref.at[place(k)], w_all.at[k], load.at[1 + nz + k]))
    loads.append(pltpu.make_async_copy(mod_ref, m_all.at[0], load.at[1 + 2 * nz]))
    loads.append(pltpu.make_async_copy(dat_ref, dat, load.at[2 + 2 * nz]))

    def split(x):
        high = x.astype(jnp.bfloat16).astype(jnp.float32)
        rest = x - high
        mid = rest.astype(jnp.bfloat16).astype(jnp.float32)
        return high, mid, rest - mid

    def station_side(ref, base):
        axis = lax.broadcasted_iota(jnp.int32, (3, half), 0)
        s = ref[...] - jnp.where(axis == 2, MID_Z, MID_XY)
        high, mid, low = (-2.0 * part for part in split(s))
        length = split(jnp.sum(s * s, axis=0, keepdims=True))
        one = jnp.ones((1, half), jnp.float32)
        zero = jnp.zeros((1, half), jnp.float32)
        rows = [high, one, *length, one, high, one, mid, zero]
        rows += [mid, zero, high, zero, low, zero, mid, zero]
        lhs[pl.ds(base, half), :] = jnp.concatenate(rows, axis=0).T.astype(jnp.bfloat16)
        for part in range(half // LANES):
            row = ref[2:3, part * LANES : (part + 1) * LANES]
            at = pl.multiple_of(base + part * LANES, LANES)
            z_col[pl.ds(at, LANES), :] = jnp.broadcast_to(row, (LANES, LANES)).T

    def cell_side(k):
        x_pad[k % 2, 0:3, :] = cel[k]
        x_pad[k % 2, 4:7, :] = cel[k]
        row = lax.broadcasted_iota(jnp.int32, (8, PIECE), 0)
        mid_of = jnp.where(row % 4 == 2, MID_Z, jnp.where(row % 4 == 3, 0.0, MID_XY))
        x = x_pad[k % 2] - mid_of
        square = x * x
        square = square + pltpu.roll(square, 1, 0)
        high, mid, low = split(x)
        length = split(square + pltpu.roll(square, 2, 0))
        first = row < 4
        last = row % 4 == 3
        parts = [
            jnp.where(last, jnp.where(first, length[0], length[1]), jnp.where(first, high, 1.0)),
            jnp.where(first, jnp.where(last, length[2], mid), high),
            jnp.where(first, mid, low),
            jnp.where(first, high, low),
        ]
        rhs[k] = jnp.concatenate(parts, axis=0).astype(jnp.bfloat16)

    def distances(k, base, buf):
        buf[...] = jnp.dot(lhs[pl.ds(base, half), :], rhs[k], preferred_element_type=jnp.float32)

    def kernel_of(k, base, buf):
        for t in range(ROWS):
            lanes = slice(t * LANES, (t + 1) * LANES)
            dz = z_col[pl.ds(base, half), :] - cel[k, 2:3, lanes]
            inv = lax.rsqrt(buf[:, lanes])
            tile[k, pl.ds(base, half), lanes] = (dz * inv) * (inv * inv)

    def generate(base, first, count, after):
        bufs = (near, far)
        for i in range(count):
            ahead = (first + i + 1, base) if i < count - 1 else after
            distances(*ahead, bufs[(i + 1) % 2])
            kernel_of(first + i, base, bufs[i % 2])

    near_first = sorted(range(1, nz), key=lambda d: min(d, nz - d))

    def forward(vector):
        acc[...] = jnp.zeros_like(acc)
        for k in (0, *near_first):
            value = vector(k)
            v_all[...] = w_all[k] * value
            vec = [jnp.broadcast_to(v_all[t : t + 1, :], (8, LANES)) for t in range(ROWS)]

            def group(i, _, k=k, vec=vec):
                rows = pl.ds(pl.multiple_of(i * 8, 8), 8)
                acc[rows, :] += tree_sum(
                    [
                        tile[k, rows, t * LANES : (t + 1) * LANES] * vec[t]
                        for t in range(ROWS)
                    ]
                )
                return 0

            lax.fori_loop(0, groups, group, 0, unroll=32)
        return [
            jnp.sum(acc[s * LANES : (s + 1) * LANES, :].T, axis=0, keepdims=True)
            for s in range(srows)
        ]

    def taken(buf, group):
        def vector(k):
            if k:
                pltpu.make_async_copy(buf.at[k], buf.at[k], pieces.at[group, k]).wait()
            return buf[k]

        return vector

    def spread(vec):
        for s in range(srows):
            rcol[s * LANES : (s + 1) * LANES, :] = jnp.broadcast_to(
                vec[s : s + 1, :], (LANES, LANES)
            ).T

    def backward(k):
        def group(i, sums):
            rows = pl.ds(pl.multiple_of(i * 8, 8), 8)
            r = rcol[rows, :]
            return tuple(
                sums[t] + tile[k, rows, t * LANES : (t + 1) * LANES] * r for t in range(ROWS)
            )

        zero = jnp.zeros((8, LANES), jnp.float32)
        sums = lax.fori_loop(0, groups, group, (zero,) * ROWS, unroll=32)
        for t in range(ROWS):
            rs_out[k, t : t + 1, :] = jnp.sum(sums[t], axis=0, keepdims=True)

    def reduce_to_owner(buf, sem):
        order = sorted(range(1, nz), key=lambda d: -min(d, nz - d))
        for k in order:
            backward(k)
            put(rs_out.at[k], buf.at[k], sem, (z + nz - k) % nz * npl + q)
        backward(0)
        arrived(others(buf), sem)
        total = rs_out[0]
        for k in range(1, nz):
            total = total + buf[k]
        left(others(rs_out), sem)
        return w_all[0] * total

    for copy in loads:
        copy.start()
    barrier = pltpu.get_barrier_semaphore()
    for d in sorted(range(1, nz), key=lambda d: -min(d, nz - d)):
        pl.semaphore_signal(barrier, inc=1, device_id=z_peer(d), device_id_type=LOGICAL)
    for d in far_first:
        pl.semaphore_signal(barrier, inc=1, device_id=plane_peer(d), device_id_type=LOGICAL)
    for i in range(2):
        for row in (3, 7):
            x_pad[i, row : row + 1, :] = jnp.full((1, PIECE), math.sqrt(SOFT), jnp.float32)
    base = pl.multiple_of(core * half, half)
    loads[0].wait()
    station_side(sta, base)
    for k in range(nz):
        loads[1 + k].wait()
    cell_side(0)
    distances(0, base, near)
    for k in range(1, nz):
        cell_side(k)
    generate(base, 0, nz // 2, (nz // 2, base))
    for copy in loads[1 + nz :]:
        copy.wait()
    pad[...] = jnp.zeros_like(pad)
    pad[0:1, 0:own_len] = dat[...]
    first = q * own_len
    mine = lax.broadcasted_iota(jnp.int32, (srows, LANES), 0) == first // LANES
    own = pltpu.roll(pad[...], first % LANES, 1)[0:1, :]
    p1[0] = jnp.where(mine, own, 0.0)
    w_all[...] = w_all[...] * scale
    pl.semaphore_wait(barrier, npl - 1 + nz - 1)
    put(sta, other, 0, plane_peer(nx * ny))
    over_z(m_all, 1, 0)
    base_2 = pl.multiple_of((1 - core) * half, half)
    generate(base, nz // 2, nz // 4, (nz // 2 + nz // 4, base))
    arrived(other, 0)
    station_side(other, base_2)
    generate(base, nz // 2 + nz // 4, nz // 4, (0, base_2))

    def half_of(j, _):
        generate(base_2, j * (nz // 2), nz // 2, ((j + 1) % 2 * (nz // 2), base_2))
        return 0

    lax.fori_loop(0, 2, half_of, 0)

    image = jnp.concatenate(forward(taken(m_all, 0)), axis=0)
    p1[0] = p1[0] - image
    over_plane(p1, 2)
    arrived(others(p1), 2)
    res = jnp.sum(p1[...], axis=0)

    spread(res)
    grad = reduce_to_owner(rs1, 3)
    g_all[0] = grad
    over_z(g_all, 4, 1, 1)

    rows = forward(taken(g_all, 1))
    grads = g_all[...]
    square = jnp.sum(jnp.sum(grads * grads, axis=0), axis=0, keepdims=True)
    p2[0] = jnp.concatenate(rows + [square], axis=0)
    over_plane(p2, 5)
    arrived(others(p2), 5)
    total = jnp.sum(p2[...], axis=0)
    image = total[0:srows]
    gamma = jnp.sum(total[srows : srows + 1], axis=1, keepdims=True)
    dl[0] = jnp.sum(image * image, axis=0, keepdims=True)
    over_z(dl, 6)

    spread(image)
    turn = reduce_to_owner(rs2, 7)
    arrived(others(dl), 6)
    delta = jnp.sum(jnp.sum(dl[...], axis=0), axis=1, keepdims=True)
    alpha = gamma / delta
    grad_next = grad - alpha * turn
    sc[0:1, :] = jnp.sum(grad_next * grad_next, axis=0, keepdims=True)

    def scalars(j, _):
        dz = far_along_z(j)

        def to(d):
            peer = (z + dz) % nz * npl + plane_peer(d) - z * npl
            put(sc.at[pl.ds(0, 1)], sc.at[pl.ds(dz * npl + d, 1)], 8, peer)

        for d in far_first:
            to(d)
        pl.when(dz > 0)(lambda: to(0))
        return 0

    lax.fori_loop(0, nz, scalars, 0)
    model_out[...] = m_all[0] + alpha * grad
    res_next = jnp.where(mine, res - alpha * image, 0.0)
    pad[0:1, :] = jnp.sum(res_next, axis=0, keepdims=True)
    res_out[...] = pltpu.roll(pad[...], (LANES - first % LANES) % LANES, 1)[0:1, :own_len]
    arrived(others(sc), 8)
    gamma_next = jnp.sum(jnp.sum(sc[...], axis=0, keepdims=True), axis=1, keepdims=True)
    search_out[...] = grad_next + gamma_next / gamma * grad

    left(other, 0)
    for buf, sem in ((m_all, 1), (p1, 2), (g_all, 4), (p2, 5), (dl, 6), (sc, 8)):
        left(others(buf), sem)


def write_out(model, res, search, model_out, res_out, search_out, sem):
    pairs = ((model, model_out), (res, res_out), (search, search_out))
    copies = [pltpu.make_async_copy(a, b, sem.at[i]) for i, (a, b) in enumerate(pairs)]
    for copy in copies:
        copy.start()
    for copy in copies:
        copy.wait()


def solution(mesh):
    shape = mesh.devices.shape
    nx = ny = math.isqrt(shape[1])
    nz = shape[0] // 2
    torus = Mesh(
        mesh.devices.reshape(nz, 2, nx, ny), ("sta_0", "sta_1", "cell_0", "cell_1")
    )

    npl = 2 * shape[1]

    def per_device(station_xyz, cell_xyz, cell_weight, data, model_start):
        half = station_xyz.shape[1]
        stations, srows = 2 * half, 2 * half // LANES
        own_len = data.shape[0]
        scale = 1.0 / math.sqrt(half * 2 * nz * cell_xyz.shape[1] * nx * ny)
        vmem = pl.BlockSpec(memory_space=pltpu.VMEM)
        f32 = jnp.float32
        cells = pltpu.VMEM((nz, ROWS, LANES), f32)
        shapes = (
            jax.ShapeDtypeStruct((ROWS, LANES), f32),
            jax.ShapeDtypeStruct((1, own_len), f32),
            jax.ShapeDtypeStruct((ROWS, LANES), f32),
        )
        results = pl.pallas_call(
            functools.partial(body, nz, nx, ny, half, own_len, scale),
            out_shape=tuple(pltpu.VMEM(x.shape, x.dtype) for x in shapes),
            in_specs=[pl.BlockSpec(memory_space=pltpu.HBM)] * 5,
            out_specs=(vmem,) * 3,
            scratch_shapes=[
                pltpu.VMEM((nz, stations, PIECE), f32),
                pltpu.VMEM((stations, 32), jnp.bfloat16),
                pltpu.VMEM((nz, 32, PIECE), jnp.bfloat16),
                pltpu.VMEM((half, PIECE), f32),
                pltpu.VMEM((half, PIECE), f32),
                pltpu.VMEM((2, 8, PIECE), f32),
                pltpu.VMEM((stations, LANES), f32),
                pltpu.VMEM((stations, LANES), f32),
                pltpu.VMEM((stations, LANES), f32),
                pltpu.VMEM((3, half), f32),
                pltpu.VMEM((3, half), f32),
                pltpu.VMEM((nz, 3, PIECE), f32),
                pltpu.VMEM((1, own_len), f32),
                cells,
                pltpu.VMEM((ROWS, LANES), f32),
                cells,
                pltpu.VMEM((npl, srows, LANES), f32),
                cells,
                cells,
                cells,
                pltpu.VMEM((npl, srows + 1, LANES), f32),
                pltpu.VMEM((nz, 1, LANES), f32),
                cells,
                pltpu.VMEM((nz * npl, LANES), f32),
                pltpu.VMEM((8, LANES), f32),
                pltpu.SemaphoreType.DMA((10,)),
                pltpu.SemaphoreType.DMA((10,)),
                pltpu.SemaphoreType.DMA((2, nz)),
                pltpu.SemaphoreType.DMA((2 * nz + 3,)),
            ],
            compiler_params=pltpu.CompilerParams(
                collective_id=0,
                has_side_effects=True,
                vmem_limit_bytes=56 * 1024 * 1024,
            ),
            name="cgls",
        )(
            station_xyz,
            cell_xyz,
            cell_weight.reshape(-1, ROWS, LANES),
            data.reshape(1, own_len),
            model_start.reshape(ROWS, LANES),
        )
        model, res, search = pl.pallas_call(
            write_out,
            out_shape=shapes,
            in_specs=[vmem] * 3,
            out_specs=(pl.BlockSpec(memory_space=pltpu.HBM),) * 3,
            scratch_shapes=[pltpu.SemaphoreType.DMA((3,))],
            name="write_out",
        )(*(pltpu.with_memory_space_constraint(x, pltpu.VMEM) for x in results))
        return model.reshape(-1), res.reshape(-1), search.reshape(-1)

    in_specs = (P(None, STA), P(None, CELL), P(CELL), P(STA_CELL), P(CELL_STA))
    out_specs = (P(CELL_STA), P(STA_CELL), P(CELL_STA))
    return jax.shard_map(
        per_device, mesh=torus, in_specs=in_specs, out_specs=out_specs, check_vma=False
    )
```
